256 devices in a mesh: groups: 4 (over x, y), rows: 64 (over z, core).
Axes of the slice: x: 2, y: 2, z: 32, core: 2. Of those that a mesh axis runs over, the one named last changes fastest.
The devices are a block of a 4x8x32 slice.
Arguments:
- phase: float32 [4096, 2048], P(('groups', 'rows')), parts along dimension 0, may hold values from -3.140625 to 3.140625
Outputs:
- filtered: float32 [2, 4096, 2048], P(None, ('groups', 'rows')), parts along dimension 1
- profile: float32 [12, 16], P('groups'), parts along dimension 0
The draws below stay inside these ranges and needn't reach their ends.
There are 4 independent parts, one for each index of `groups`. The reference program is written for one: setup_inputs(seed, part) draws one part's arguments, and reference() takes and returns one part's arrays. A program takes and returns all parts, laid end to end along the dimension named above; each array names one. Nothing has to cross between parts.
All inputs are finite; a program needn't handle non-finite values.
Results may differ from the reference program's by a relative error of at most 0.00012.
Values sent between devices are 32-bit elements; how exact they have to be, the bound alone decides.
A program may use at most 64 MiB of HBM per device.

```python
import jax
import jax.numpy as jnp
from jax import lax

COLS = 2048
ITERS = 3
NR = 1024


def setup_inputs(seed: int = 0, part: int = 0) -> dict:
    streams_of = jax.random.split(jax.random.key(seed), 2)
    part_splits = jax.random.split(jax.random.fold_in(streams_of[1], part), 2)
    phase = jnp.clip(jax.random.uniform(part_splits[0], (NR, COLS), jnp.float32, -3.140625, 3.140625), -3.140625, 3.140625)
    return {"phase": phase}


EPS = 1e-6


def residue_sums(padded_rows):
    padded = jnp.pad(padded_rows, ((0, 0), (0, 0), (0, 1)))
    first = padded[:, :-1, :-1]
    second = padded[:, :-1, 1:]
    third = padded[:, 1:, 1:]
    fourth = padded[:, 1:, :-1]

    def cross(left, right):
        return left[1] * right[0] - left[0] * right[1]

    loop = cross(first, second) + cross(second, third) + cross(third, fourth) + cross(fourth, first)
    height = loop.shape[0]
    return jnp.sum((loop * loop).reshape(height, COLS // 128, 128), axis=(0, 2))


def goldstein(field, taper):
    extended = jnp.pad(field, ((0, 0), (0, 16), (0, 16)))
    blocks = extended.reshape(2, NR // 16 + 1, 16, COLS // 16 + 1, 16)

    def one_row(start):
        strip = lax.dynamic_slice_in_dim(blocks, start, 2, 1).reshape(2, 32, COLS // 16 + 1, 16)
        windows = jnp.concatenate([strip[:, :, :-1], strip[:, :, 1:]], axis=3)
        signal = windows[0] + 1j * windows[1]
        spectrum = jnp.fft.fft2(signal, axes=(0, 2))
        power = spectrum.real ** 2 + spectrum.imag ** 2
        average = jnp.mean(power, axis=(0, 2), keepdims=True)
        result = jnp.fft.ifft2(spectrum * (power / (average + EPS)) ** 0.25, axes=(0, 2)) * taper
        return jnp.stack([result.real, result.imag])

    pieces = lax.map(one_row, jnp.arange(NR // 16, dtype=jnp.int32))
    righty = jnp.pad(pieces[..., 16:], ((0, 0), (0, 0), (0, 0), (1, 0), (0, 0)))[:, :, :, :-1]
    columns = (pieces[..., :16] + righty).reshape(NR // 16, 2, 32, COLS)
    lower = jnp.pad(columns[:, :, 16:], ((1, 0), (0, 0), (0, 0), (0, 0)))[:-1]
    joined = columns[:, :, :16] + lower
    return joined.transpose(1, 0, 2, 3).reshape(2, NR, COLS)


def reference(phase):
    field = jnp.stack([jnp.cos(phase), jnp.sin(phase)])
    offsets = jnp.arange(32, dtype=jnp.float32)
    ramp = 1.0 - jnp.abs(offsets - 15.5) / 16.0
    taper = ramp[:, None, None] * ramp[None, None, :]
    reports = []
    for step in range(ITERS):
        padded_rows = jnp.pad(field, ((0, 0), (0, 1), (0, 0)))
        reports.append(residue_sums(padded_rows) / (NR * 128.0))
        field = goldstein(field, taper)
    return field, jnp.stack(reports)
```

```python
import functools
import math

import jax
import jax.numpy as jnp
import numpy as np
from jax import lax
from jax.experimental import pallas as pl
from jax.experimental.pallas import tpu as pltpu
from jax.sharding import PartitionSpec as P

ITERS = 3
EPS = 1e-06
WIN = 32
HALF = 16
LANES = 128
F32 = jnp.float32
BF16 = jnp.bfloat16
MESH = pl.DeviceIdType.MESH

PHASE_ENDS = (7, 12, 16)
CHUNK_ENDS = ((6, 11, 16), (5, 10, 16), (4, 9, 16))


def hi_lo(table):
    high = table.astype(np.float32).astype(jnp.bfloat16)
    low = (table - high.astype(np.float64)).astype(np.float32).astype(jnp.bfloat16)
    return high, low


def tables():
    counter = np.arange(WIN)
    angles = 2.0 * math.pi / WIN * (counter[:, None] * counter[None, :] % WIN)
    cos, sin = np.cos(angles), np.sin(angles)
    ramp = 1.0 - np.abs(counter - 15.5) / 16.0

    def rows(real, imag):
        return np.concatenate([real[:HALF], imag[:HALF], real[HALF:], imag[HALF:]])

    forward = np.concatenate(
        [rows(cos.T, sin.T).T, rows(-sin.T, cos.T).T], axis=0
    )
    high, low = hi_lo(forward)
    row_in = np.concatenate([high, high, low], axis=1)
    scale = ramp[:, None] / WIN
    backward = rows(
        np.concatenate([cos, -sin], axis=1) * scale, np.concatenate([sin, cos], axis=1) * scale
    )
    high, low = hi_lo(backward)
    row_out = np.concatenate([high, high, low], axis=1)
    four = np.eye(LANES // WIN)
    c, s = np.kron(four, cos), np.kron(four, sin)
    high, low = hi_lo(np.block([[c, -s], [s, c]]))
    col_in = np.concatenate([high, high, low], axis=0)
    taper = np.tile(ramp, LANES // WIN)[None, :] / WIN
    high, low = hi_lo(np.block([[c * taper, s * taper], [-s * taper, c * taper]]))
    col_out = np.concatenate([high, high, low], axis=0)
    ones = np.kron(four, np.ones((WIN, WIN)))
    ones = np.concatenate([ones, ones], axis=0).astype(jnp.bfloat16)
    return [row_in, col_in, col_out, row_out, ones]


def split(x):
    high = x.astype(BF16)
    return high, (x - high.astype(F32)).astype(BF16)


def split_rows(x):
    high, low = split(x)
    return jnp.concatenate([high, low, high], axis=0)


def split_cols(x):
    high, low = split(x)
    return jnp.concatenate([high, low, high], axis=1)


def dot(a, b):
    return jnp.dot(a, b, preferred_element_type=F32)


def unit(phase):
    y = phase * 0.5
    t = y * y
    sine = -1.0 / 39916800.0
    for c in (1.0 / 362880.0, -1.0 / 5040.0, 1.0 / 120.0, -1.0 / 6.0, 1.0):
        sine = sine * t + c
    sine = sine * y
    cosine = 1.0 / 479001600.0
    for c in (-1.0 / 3628800.0, 1.0 / 40320.0, -1.0 / 720.0, 1.0 / 24.0, -0.5, 1.0):
        cosine = cosine * t + c
    return 1.0 - 2.0 * (sine * sine), 2.0 * (sine * cosine)


def to_lanes(tiles):
    return jnp.concatenate([tiles[j] for j in range(tiles.shape[0])], axis=1)


def to_tiles(wide):
    return jnp.stack(
        [wide[:, LANES * j : LANES * (j + 1)] for j in range(wide.shape[1] // LANES)]
    )


def kernel(
    n,
    tiles,
    phase_hbm,
    row_in_hbm,
    col_in_hbm,
    col_out_hbm,
    row_out_hbm,
    ones_hbm,
    out_hbm,
    prof_ref,
    phase,
    row_in,
    col_in,
    col_out,
    row_out,
    ones,
    x,
    eo,
    rv,
    carry,
    zout,
    pay_a,
    pay_b,
    got_a,
    got_b,
    load_sem,
    ph_send,
    ph_recv,
    up_send,
    up_recv,
    dn_send,
    dn_recv,
    a_send,
    a_recv,
    b_send,
    b_recv,
    out_sem,
    relay,
):
    me = lax.axis_index("rows")
    has_above = me > 0
    has_below = me < n - 1

    def ring(offset):
        return {"rows": lax.rem(me + (offset + n), n)}

    def greet(sem, distance):
        for offset in (-distance, distance):
            pl.semaphore_signal(sem, inc=1, device_id=ring(offset), device_id_type=MESH)

    barrier = pltpu.get_barrier_semaphore()
    greet(barrier, 1)

    loads = [
        pltpu.make_async_copy(src, dst, load_sem.at[i])
        for i, (src, dst) in enumerate(
            [
                (phase_hbm, phase.at[0]),
                (row_in_hbm, row_in),
                (ones_hbm, ones),
                (col_in_hbm, col_in),
                (col_out_hbm, col_out),
                (row_out_hbm, row_out),
            ]
        )
    ]
    for load in loads:
        load.start()

    keep_below = jnp.where(has_below, 1.0, 0.0).astype(F32)

    @pl.when(jnp.logical_not(has_above))
    def _():
        rv[:, 0] = jnp.zeros(rv.shape[:1] + rv.shape[2:], F32)

    @pl.when(jnp.logical_not(has_below))
    def _():
        rv[:, 1] = jnp.zeros(rv.shape[:1] + rv.shape[2:], F32)
        phase[1] = jnp.zeros(phase.shape[1:], F32)

    x[tiles] = jnp.zeros(x.shape[1:], F32)
    loads[0].wait()
    pl.semaphore_wait(barrier, 2)

    stages = relay.shape[0]
    greet(relay.at[0], 1)

    def relay_step(s):
        if s < stages:
            pl.semaphore_wait(relay.at[s], 2)
            if s + 1 < stages:
                greet(relay.at[s + 1], 2 ** (s + 1))

    def phase_copy(c):
        first = PHASE_ENDS[c - 1] if c else 0
        cols = pl.ds(first * LANES, (PHASE_ENDS[c] - first) * LANES)
        return pltpu.make_async_remote_copy(
            src_ref=phase.at[0, :, cols],
            dst_ref=phase.at[1, :, cols],
            send_sem=ph_send.at[c],
            recv_sem=ph_recv.at[c],
            device_id={"rows": jnp.maximum(me - 1, 0)},
            device_id_type=MESH,
        )

    def span(it, c):
        ends = CHUNK_ENDS[it]
        return (ends[c - 1] if c else 0), ends[c]

    def up_copy(it, c):
        lo, hi = span(it, c)
        return pltpu.make_async_remote_copy(
            src_ref=eo.at[it, 0, pl.ds(lo, hi - lo)],
            dst_ref=rv.at[it, 1, pl.ds(lo, hi - lo)],
            send_sem=up_send.at[it, c],
            recv_sem=up_recv.at[it, c],
            device_id={"rows": jnp.maximum(me - 1, 0)},
            device_id_type=MESH,
        )

    def dn_copy(it, c):
        lo, hi = span(it, c)
        return pltpu.make_async_remote_copy(
            src_ref=eo.at[it, 1, pl.ds(lo, hi - lo)],
            dst_ref=rv.at[it, 0, pl.ds(lo, hi - lo)],
            send_sem=dn_send.at[it, c],
            recv_sem=dn_recv.at[it, c],
            device_id={"rows": jnp.minimum(me + 1, n - 1)},
            device_id_type=MESH,
        )

    @pl.when(has_above)
    def _():
        for c in range(len(PHASE_ENDS)):
            phase_copy(c).start()

    lane = lax.broadcasted_iota(jnp.int32, (1, 1, LANES), 2)

    def unit_tiles(row, lo, hi, scale=None):
        real, imag = unit(phase[row, :, lo * LANES : hi * LANES])
        if scale is not None:
            real, imag = real * scale, imag * scale
        return to_tiles(jnp.concatenate([real, imag], axis=0))

    x[0:tiles, 0:WIN] = unit_tiles(0, 0, tiles)
    for load in loads[1:]:
        load.wait()
    below_rows = lax.broadcasted_iota(jnp.int32, row_out.shape, 0) >= WIN
    row_out[...] = jnp.where(
        jnp.logical_and(below_rows, jnp.logical_not(has_below)),
        jnp.zeros(row_out.shape, BF16),
        row_out[...],
    )

    def arrive(it, c):
        if it == 0:
            lo, hi = (PHASE_ENDS[c - 1] if c else 0), PHASE_ENDS[c]

            @pl.when(has_above)
            def _():
                phase_copy(c).wait_send()

            @pl.when(has_below)
            def _():
                phase_copy(c).wait_recv()

            x[lo:hi, WIN:] = unit_tiles(1, lo, hi, keep_below)
            return hi
        lo, hi = span(it - 1, c)

        @pl.when(has_above)
        def _():
            up_copy(it - 1, c).wait_send()
            dn_copy(it - 1, c).wait_recv()

        @pl.when(has_below)
        def _():
            up_copy(it - 1, c).wait_recv()
            dn_copy(it - 1, c).wait_send()

        x[lo:hi] = jnp.concatenate(
            [eo[it - 1, 0, lo:hi] + rv[it - 1, 0, lo:hi], eo[it - 1, 1, lo:hi] + rv[it - 1, 1, lo:hi]],
            axis=1,
        )
        return hi

    def residues(it, lo, hi):
        field = x[lo : hi + 1]
        last_row = lax.broadcasted_iota(jnp.int32, (1, HALF, 1), 1) == HALF - 1

        def lower(a, b):
            return jnp.where(last_row, b[:, 0:1], pltpu.roll(a, HALF - 1, 1))

        def right(a):
            return pltpu.roll(jnp.where(lane == 0, a[1:], a[:-1]), LANES - 1, 2)

        ar, ai = field[:, 0:HALF], field[:, HALF:WIN]
        dr = lower(ar, field[:, WIN : WIN + HALF])
        di = lower(ai, field[:, WIN + HALF :])
        pr, pi = ar[:-1] - right(dr), ai[:-1] - right(di)
        qr, qi = right(ar) - dr[:-1], right(ai) - di[:-1]
        loop = pi * qr - pr * qi
        loop = loop * loop
        loop = loop[:, 0:8] + loop[:, 8:HALF]
        sums = jnp.sum(loop, axis=2, keepdims=True)
        lanes = lax.broadcasted_iota(jnp.int32, (8, LANES), 1)
        total = jnp.zeros((8, LANES), F32)
        for j in range(hi - lo):
            total = jnp.where(lanes == it * tiles + lo + j, sums[j], total)
        return total

    def windows(it, lo, hi):
        count = hi - lo
        field = x[lo : hi + 1]
        y = to_tiles(dot(row_in[...], split_rows(to_lanes(field))))
        square = field * field
        square = sum(square[:, 8 * i : 8 * i + 8] for i in range(8))

        def both(tall):
            odd = pltpu.roll(jnp.where(lane < HALF, tall[1:], tall[:-1]), LANES - HALF, 2)
            return jnp.concatenate([tall[:-1], odd], axis=0)

        high, low = split(both(square).reshape(2 * count * 8, LANES))
        mean = dot(jnp.concatenate([high, low], axis=1), ones[...])
        mean = jnp.sum(mean.reshape(2 * count, 8, LANES), axis=1, keepdims=True)
        inverse = 1.0 / (mean + EPS)

        y = both(y)
        y = jnp.concatenate([y[:, 0:WIN], y[:, WIN:]], axis=2).reshape(2 * count * WIN, 2 * LANES)
        s = dot(split_cols(y), col_in[...]).reshape(2 * count, WIN, 2 * LANES)
        sr, si = s[:, :, 0:LANES], s[:, :, LANES:]
        gain = lax.rsqrt(lax.rsqrt((sr * sr + si * si) * inverse))
        s = jnp.concatenate([sr * gain, si * gain], axis=2).reshape(2 * count * WIN, 2 * LANES)
        s = dot(split_cols(s), col_out[...]).reshape(2 * count, WIN, 2 * LANES)
        s = jnp.concatenate([s[:, :, 0:LANES], s[:, :, LANES:]], axis=1)
        moved = pltpu.roll(s[count:], HALF, 2)
        if lo == 0:
            before = jnp.zeros((1, 2 * WIN, LANES), F32)
        else:
            before = carry[...][None]
        if hi < tiles:
            carry[...] = moved[count - 1]
        before = jnp.concatenate([before, moved[:-1]], axis=0)
        s = s[:count] + jnp.where(lane < HALF, before, moved)
        result = to_tiles(dot(row_out[...], split_rows(to_lanes(s))))
        eo[it, 0, lo:hi] = result[:, 0:WIN]
        eo[it, 1, lo:hi] = result[:, WIN:]

    group = a_send.shape[0] + 1
    a_offsets = [o for o in range(-(group // 2), group - group // 2) if o]
    b_offsets = [group * j for j in range(1, n // group)]

    def a_copy(i):
        return pltpu.make_async_remote_copy(
            src_ref=pay_a,
            dst_ref=got_a.at[i],
            send_sem=a_send.at[i],
            recv_sem=a_recv.at[i],
            device_id=ring(a_offsets[i]),
            device_id_type=MESH,
        )

    def b_copy(i):
        return pltpu.make_async_remote_copy(
            src_ref=pay_b,
            dst_ref=got_b.at[i],
            send_sem=b_send.at[i],
            recv_sem=b_recv.at[i],
            device_id=ring(b_offsets[i]),
            device_id_type=MESH,
        )

    chunks = len(PHASE_ENDS)
    payload = jnp.zeros((8, LANES), F32)
    done_stages = 0
    for it in range(ITERS):
        last = it == ITERS - 1
        if last:
            for c in range(chunks):
                arrive(it, c)
            payload = payload + residues(it, 0, tiles)
            pay_a[...] = jnp.sum(payload, axis=0, keepdims=True)
            for i in range(len(a_offsets)):
                a_copy(i).start()
        for c in range(chunks):
            lo, hi = span(it, c)
            if not last:
                arrive(it, c)
                payload = payload + residues(it, lo, hi)
            windows(it, lo, hi)
            if not last:

                @pl.when(has_above)
                def _():
                    up_copy(it, c).start()

            @pl.when(has_below)
            def _():
                dn_copy(it, c).start()

            if it * chunks + c < 4 and done_stages < stages:
                relay_step(done_stages)
                done_stages += 1
    while done_stages < stages:
        relay_step(done_stages)
        done_stages += 1

    total = pay_a[...]
    for i in range(len(a_offsets)):
        a_copy(i).wait()
        total = total + got_a[i]
    pay_b[...] = total
    for i in range(len(b_offsets)):
        b_copy(i).start()

    for c in range(chunks):
        lo, hi = span(ITERS - 1, c)

        @pl.when(has_above)
        def _():
            dn_copy(ITERS - 1, c).wait_recv()

        @pl.when(has_below)
        def _():
            dn_copy(ITERS - 1, c).wait_send()

        final = to_lanes(eo[ITERS - 1, 0, lo:hi] + rv[ITERS - 1, 0, lo:hi])
        zout[0, :, lo * LANES : hi * LANES] = final[0:HALF]
        zout[1, :, lo * LANES : hi * LANES] = final[HALF:]
    store = pltpu.make_async_copy(zout, out_hbm, out_sem)
    store.start()

    for i in range(len(b_offsets)):
        b_copy(i).wait()
        total = total + got_b[i]
    total = total * (1.0 / (n * HALF * LANES))
    for it in range(ITERS):
        moved = total if it == 0 else pltpu.roll(total, LANES - it * tiles, 1)
        prof_ref[it : it + 1, :] = moved[:, 0:tiles]
    store.wait()


def per_device(phase):
    n = lax.axis_size("rows")
    height, width = phase.shape
    tiles = width // LANES
    consts = [jnp.asarray(t) for t in tables()]
    stages = max(1, int(math.log2(n)) - 1)
    group = 8
    far = n // group - 1
    chunks = len(PHASE_ENDS)
    dma = pltpu.SemaphoreType.DMA
    any_spec = pl.BlockSpec(memory_space=pl.ANY)
    return pl.pallas_call(
        functools.partial(kernel, n, tiles),
        out_shape=(
            jax.ShapeDtypeStruct((2, height, width), F32),
            jax.ShapeDtypeStruct((ITERS, tiles), F32),
        ),
        in_specs=[any_spec] * 6,
        out_specs=(any_spec, pl.BlockSpec(memory_space=pltpu.VMEM)),
        scratch_shapes=[
            pltpu.VMEM((2, height, width), F32),
            *[pltpu.VMEM(c.shape, c.dtype) for c in consts[:4]],
            pltpu.VMEM(consts[4].shape, consts[4].dtype),
            pltpu.VMEM((tiles + 1, 2 * WIN, LANES), F32),
            pltpu.VMEM((ITERS, 2, tiles, WIN, LANES), F32),
            pltpu.VMEM((ITERS, 2, tiles, WIN, LANES), F32),
            pltpu.VMEM((2 * WIN, LANES), F32),
            pltpu.VMEM((2, height, width), F32),
            pltpu.VMEM((1, LANES), F32),
            pltpu.VMEM((1, LANES), F32),
            pltpu.VMEM((group - 1, 1, LANES), F32),
            pltpu.VMEM((far, 1, LANES), F32),
            dma((6,)),
            dma((chunks,)),
            dma((chunks,)),
            dma((ITERS, chunks)),
            dma((ITERS, chunks)),
            dma((ITERS, chunks)),
            dma((ITERS, chunks)),
            dma((group - 1,)),
            dma((group - 1,)),
            dma((far,)),
            dma((far,)),
            dma,
            pltpu.SemaphoreType.REGULAR((stages,)),
        ],
        compiler_params=pltpu.CompilerParams(
            collective_id=0, has_side_effects=True, vmem_limit_bytes=60 << 20
        ),
        name="goldstein",
    )(phase, *consts)


def solution(mesh):
    return jax.shard_map(
        per_device,
        mesh=mesh,
        in_specs=(P(("groups", "rows"), None),),
        out_specs=(P(None, ("groups", "rows"), None), P("groups", None)),
        check_vma=False,
    )
```

```python
import functools
import math

import jax
import jax.numpy as jnp
import numpy as np
from jax import lax
from jax.experimental import pallas as pl
from jax.experimental.pallas import tpu as pltpu
from jax.sharding import PartitionSpec as P

ITERS = 3
EPS = 1e-06
WIN = 32
HALF = 16
LANES = 128
F32 = jnp.float32
BF16 = jnp.bfloat16
MESH = pl.DeviceIdType.MESH
ROOTS = 4

PHASE_ENDS = (7, 12, 16)
CHUNK_ENDS = ((6, 11, 16), (5, 10, 16), (4, 9, 16))


def hi_lo(table):
    high = table.astype(np.float32).astype(jnp.bfloat16)
    low = (table - high.astype(np.float64)).astype(np.float32).astype(jnp.bfloat16)
    return high, low


def tables():
    counter = np.arange(WIN)
    angles = 2.0 * math.pi / WIN * (counter[:, None] * counter[None, :] % WIN)
    cos, sin = np.cos(angles), np.sin(angles)
    ramp = 1.0 - np.abs(counter - 15.5) / 16.0

    def rows(real, imag):
        return np.concatenate([real[:HALF], imag[:HALF], real[HALF:], imag[HALF:]])

    forward = np.concatenate(
        [rows(cos.T, sin.T).T, rows(-sin.T, cos.T).T], axis=0
    )
    high, low = hi_lo(forward)
    row_in = np.concatenate([high, high, low], axis=1)
    scale = ramp[:, None] / WIN
    backward = rows(
        np.concatenate([cos, -sin], axis=1) * scale, np.concatenate([sin, cos], axis=1) * scale
    )
    high, low = hi_lo(backward)
    row_out = np.concatenate([high, high, low], axis=1)
    four = np.eye(LANES // WIN)
    c, s = np.kron(four, cos), np.kron(four, sin)
    high, low = hi_lo(np.block([[c, -s], [s, c]]))
    col_in = np.concatenate([high, high, low], axis=0)
    taper = np.tile(ramp, LANES // WIN)[None, :] / WIN
    high, low = hi_lo(np.block([[c * taper, s * taper], [-s * taper, c * taper]]))
    col_out = np.concatenate([high, high, low], axis=0)
    ones = np.kron(four, np.ones((WIN, WIN)))
    ones = np.concatenate([ones, ones], axis=0).astype(jnp.bfloat16)
    return [row_in, col_in, col_out, row_out, ones]


def split(x):
    high = x.astype(BF16)
    return high, (x - high.astype(F32)).astype(BF16)


def split_rows(x):
    high, low = split(x)
    return jnp.concatenate([high, low, high], axis=0)


def split_cols(x):
    high, low = split(x)
    return jnp.concatenate([high, low, high], axis=1)


def dot(a, b):
    return jnp.dot(a, b, preferred_element_type=F32)


def unit(phase):
    y = phase * 0.5
    t = y * y
    sine = -1.0 / 39916800.0
    for c in (1.0 / 362880.0, -1.0 / 5040.0, 1.0 / 120.0, -1.0 / 6.0, 1.0):
        sine = sine * t + c
    sine = sine * y
    cosine = 1.0 / 479001600.0
    for c in (-1.0 / 3628800.0, 1.0 / 40320.0, -1.0 / 720.0, 1.0 / 24.0, -0.5, 1.0):
        cosine = cosine * t + c
    return 1.0 - 2.0 * (sine * sine), 2.0 * (sine * cosine)


def to_lanes(tiles):
    return jnp.concatenate([tiles[j] for j in range(tiles.shape[0])], axis=1)


def to_tiles(wide):
    return jnp.stack(
        [wide[:, LANES * j : LANES * (j + 1)] for j in range(wide.shape[1] // LANES)]
    )


def kernel(
    n,
    tiles,
    phase_hbm,
    row_in_hbm,
    col_in_hbm,
    col_out_hbm,
    row_out_hbm,
    ones_hbm,
    out_hbm,
    prof_ref,
    phase,
    row_in,
    col_in,
    col_out,
    row_out,
    ones,
    x,
    eo,
    rv,
    carry,
    zout,
    pay,
    got,
    answer,
    load_sem,
    ph_send,
    ph_recv,
    up_send,
    up_recv,
    dn_send,
    dn_recv,
    pay_send,
    pay_recv,
    ans_send,
    ans_recv,
    out_sem,
    relay,
):
    me = lax.axis_index("rows")
    has_above = me > 0
    has_below = me < n - 1

    def ring(offset):
        return {"rows": lax.rem(me + (offset + n), n)}

    def greet(sem, distance):
        for offset in (-distance, distance):
            pl.semaphore_signal(sem, inc=1, device_id=ring(offset), device_id_type=MESH)

    barrier = pltpu.get_barrier_semaphore()
    greet(barrier, 1)
    greet(barrier, 2)

    loads = [
        pltpu.make_async_copy(src, dst, load_sem.at[i])
        for i, (src, dst) in enumerate(
            [
                (phase_hbm, phase.at[0]),
                (row_in_hbm, row_in),
                (ones_hbm, ones),
                (col_in_hbm, col_in),
                (col_out_hbm, col_out),
                (row_out_hbm, row_out),
            ]
        )
    ]
    for load in loads:
        load.start()

    keep_below = jnp.where(has_below, 1.0, 0.0).astype(F32)

    @pl.when(jnp.logical_not(has_above))
    def _():
        rv[:, 0] = jnp.zeros(rv.shape[:1] + rv.shape[2:], F32)

    @pl.when(jnp.logical_not(has_below))
    def _():
        rv[:, 1] = jnp.zeros(rv.shape[:1] + rv.shape[2:], F32)
        phase[1] = jnp.zeros(phase.shape[1:], F32)

    x[tiles] = jnp.zeros(x.shape[1:], F32)
    loads[0].wait()
    pl.semaphore_wait(barrier, 4)

    stages = relay.shape[0]
    greet(relay.at[0], 2)

    def relay_step(s):
        if s < stages:
            pl.semaphore_wait(relay.at[s], 2)
            if s + 1 < stages:
                greet(relay.at[s + 1], 4 * 2 ** s)

    def phase_copy(c):
        first = PHASE_ENDS[c - 1] if c else 0
        cols = pl.ds(first * LANES, (PHASE_ENDS[c] - first) * LANES)
        return pltpu.make_async_remote_copy(
            src_ref=phase.at[0, :, cols],
            dst_ref=phase.at[1, :, cols],
            send_sem=ph_send.at[c],
            recv_sem=ph_recv.at[c],
            device_id={"rows": jnp.maximum(me - 1, 0)},
            device_id_type=MESH,
        )

    def span(it, c):
        ends = CHUNK_ENDS[it]
        return (ends[c - 1] if c else 0), ends[c]

    def up_copy(it, c):
        lo, hi = span(it, c)
        return pltpu.make_async_remote_copy(
            src_ref=eo.at[it, 0, pl.ds(lo, hi - lo)],
            dst_ref=rv.at[it, 1, pl.ds(lo, hi - lo)],
            send_sem=up_send.at[it, c],
            recv_sem=up_recv.at[it, c],
            device_id={"rows": jnp.maximum(me - 1, 0)},
            device_id_type=MESH,
        )

    def dn_copy(it, c):
        lo, hi = span(it, c)
        return pltpu.make_async_remote_copy(
            src_ref=eo.at[it, 1, pl.ds(lo, hi - lo)],
            dst_ref=rv.at[it, 0, pl.ds(lo, hi - lo)],
            send_sem=dn_send.at[it, c],
            recv_sem=dn_recv.at[it, c],
            device_id={"rows": jnp.minimum(me + 1, n - 1)},
            device_id_type=MESH,
        )

    @pl.when(has_above)
    def _():
        for c in range(len(PHASE_ENDS)):
            phase_copy(c).start()

    lane = lax.broadcasted_iota(jnp.int32, (1, 1, LANES), 2)

    def unit_tiles(row, lo, hi, scale=None):
        real, imag = unit(phase[row, :, lo * LANES : hi * LANES])
        if scale is not None:
            real, imag = real * scale, imag * scale
        return to_tiles(jnp.concatenate([real, imag], axis=0))

    x[0:tiles, 0:WIN] = unit_tiles(0, 0, tiles)
    for load in loads[1:]:
        load.wait()
    below_rows = lax.broadcasted_iota(jnp.int32, row_out.shape, 0) >= WIN
    row_out[...] = jnp.where(
        jnp.logical_and(below_rows, jnp.logical_not(has_below)),
        jnp.zeros(row_out.shape, BF16),
        row_out[...],
    )

    def arrive(it, c):
        if it == 0:
            lo, hi = (PHASE_ENDS[c - 1] if c else 0), PHASE_ENDS[c]

            @pl.when(has_above)
            def _():
                phase_copy(c).wait_send()

            @pl.when(has_below)
            def _():
                phase_copy(c).wait_recv()

            x[lo:hi, WIN:] = unit_tiles(1, lo, hi, keep_below)
            return hi
        lo, hi = span(it - 1, c)

        @pl.when(has_above)
        def _():
            up_copy(it - 1, c).wait_send()
            dn_copy(it - 1, c).wait_recv()

        @pl.when(has_below)
        def _():
            up_copy(it - 1, c).wait_recv()
            dn_copy(it - 1, c).wait_send()

        x[lo:hi] = jnp.concatenate(
            [eo[it - 1, 0, lo:hi] + rv[it - 1, 0, lo:hi], eo[it - 1, 1, lo:hi] + rv[it - 1, 1, lo:hi]],
            axis=1,
        )
        return hi

    def residues(it, lo, hi):
        field = x[lo : hi + 1]
        last_row = lax.broadcasted_iota(jnp.int32, (1, HALF, 1), 1) == HALF - 1

        def lower(a, b):
            return jnp.where(last_row, b[:, 0:1], pltpu.roll(a, HALF - 1, 1))

        def right(a):
            return pltpu.roll(jnp.where(lane == 0, a[1:], a[:-1]), LANES - 1, 2)

        ar, ai = field[:, 0:HALF], field[:, HALF:WIN]
        dr = lower(ar, field[:, WIN : WIN + HALF])
        di = lower(ai, field[:, WIN + HALF :])
        pr, pi = ar[:-1] - right(dr), ai[:-1] - right(di)
        qr, qi = right(ar) - dr[:-1], right(ai) - di[:-1]
        loop = pi * qr - pr * qi
        loop = loop * loop
        loop = loop[:, 0:8] + loop[:, 8:HALF]
        sums = jnp.sum(loop, axis=2, keepdims=True)
        lanes = lax.broadcasted_iota(jnp.int32, (8, LANES), 1)
        total = jnp.zeros((8, LANES), F32)
        for j in range(hi - lo):
            total = jnp.where(lanes == it * tiles + lo + j, sums[j], total)
        return total

    def windows(it, lo, hi):
        count = hi - lo
        field = x[lo : hi + 1]
        y = to_tiles(dot(row_in[...], split_rows(to_lanes(field))))
        square = field * field
        square = sum(square[:, 8 * i : 8 * i + 8] for i in range(8))

        def both(tall):
            odd = pltpu.roll(jnp.where(lane < HALF, tall[1:], tall[:-1]), LANES - HALF, 2)
            return jnp.concatenate([tall[:-1], odd], axis=0)

        high, low = split(both(square).reshape(2 * count * 8, LANES))
        mean = dot(jnp.concatenate([high, low], axis=1), ones[...])
        mean = jnp.sum(mean.reshape(2 * count, 8, LANES), axis=1, keepdims=True)
        inverse = 1.0 / (mean + EPS)

        y = both(y)
        y = jnp.concatenate([y[:, 0:WIN], y[:, WIN:]], axis=2).reshape(2 * count * WIN, 2 * LANES)
        s = dot(split_cols(y), col_in[...]).reshape(2 * count, WIN, 2 * LANES)
        sr, si = s[:, :, 0:LANES], s[:, :, LANES:]
        gain = lax.rsqrt(lax.rsqrt((sr * sr + si * si) * inverse))
        s = jnp.concatenate([sr * gain, si * gain], axis=2).reshape(2 * count * WIN, 2 * LANES)
        s = dot(split_cols(s), col_out[...]).reshape(2 * count, WIN, 2 * LANES)
        s = jnp.concatenate([s[:, :, 0:LANES], s[:, :, LANES:]], axis=1)
        moved = pltpu.roll(s[count:], HALF, 2)
        if lo == 0:
            before = jnp.zeros((1, 2 * WIN, LANES), F32)
        else:
            before = carry[...][None]
        if hi < tiles:
            carry[...] = moved[count - 1]
        before = jnp.concatenate([before, moved[:-1]], axis=0)
        s = s[:count] + jnp.where(lane < HALF, before, moved)
        result = to_tiles(dot(row_out[...], split_rows(to_lanes(s))))
        eo[it, 0, lo:hi] = result[:, 0:WIN]
        eo[it, 1, lo:hi] = result[:, WIN:]

    def pay_copy(root):
        return pltpu.make_async_remote_copy(
            src_ref=pay,
            dst_ref=got.at[lax.rem(me - root + n, n)],
            send_sem=pay_send.at[root],
            recv_sem=pay_recv,
            device_id={"rows": root},
            device_id_type=MESH,
        )

    def answer_copy(i):
        return pltpu.make_async_remote_copy(
            src_ref=answer,
            dst_ref=answer,
            send_sem=ans_send.at[i],
            recv_sem=ans_recv,
            device_id={"rows": jnp.minimum(me + ROOTS * (i + 1), n - 1)},
            device_id_type=MESH,
        )

    chunks = len(PHASE_ENDS)
    payload = jnp.zeros((8, LANES), F32)
    relay_step(0)
    for it in range(ITERS - 1):
        for c in range(chunks):
            lo, hi = span(it, c)
            arrive(it, c)
            if c == 0 and it == 0:
                relay_step(1)
            windows(it, lo, hi)

            @pl.when(has_above)
            def _():
                up_copy(it, c).start()

            @pl.when(has_below)
            def _():
                dn_copy(it, c).start()

        payload = payload + residues(it, 0, tiles)
        if it == 0:
            relay_step(2)

    last = ITERS - 1
    for c in range(chunks):
        arrive(last, c)
        payload = payload + residues(last, *span(last, c))
    pay[...] = jnp.sum(payload, axis=0, keepdims=True)
    for s in range(3, stages):
        relay_step(s)
    for root in range(ROOTS):

        @pl.when(me != root)
        def _():
            pay_copy(root).start()

    for c in range(chunks):
        windows(last, *span(last, c))

        @pl.when(has_below)
        def _():
            dn_copy(last, c).start()

    for c in range(chunks):
        lo, hi = span(last, c)

        @pl.when(has_above)
        def _():
            dn_copy(last, c).wait_recv()

        @pl.when(has_below)
        def _():
            dn_copy(last, c).wait_send()

        final = to_lanes(eo[last, 0, lo:hi] + rv[last, 0, lo:hi])
        zout[0, :, lo * LANES : hi * LANES] = final[0:HALF]
        zout[1, :, lo * LANES : hi * LANES] = final[HALF:]
    store = pltpu.make_async_copy(zout, out_hbm, out_sem)
    store.start()
    store.wait()
    for root in range(ROOTS):

        @pl.when(me != root)
        def _():
            pay_copy(root).wait_send()

    is_root = me < ROOTS
    answers = ans_send.shape[0]

    @pl.when(is_root)
    def _():
        others = got.at[pl.ds(1, n - 1)]
        pltpu.make_async_remote_copy(
            src_ref=others,
            dst_ref=others,
            send_sem=pay_send.at[0],
            recv_sem=pay_recv,
            device_id=ring(1),
            device_id_type=MESH,
        ).wait_recv()
        total = pay[...] + jnp.sum(got[1:n], axis=0)
        answer[...] = total * (1.0 / (n * HALF * LANES))
        for i in range(answers):
            answer_copy(i).start()

    @pl.when(jnp.logical_not(is_root))
    def _():
        answer_copy(0).wait_recv()

    for it in range(ITERS):
        moved = answer[...] if it == 0 else pltpu.roll(answer[...], LANES - it * tiles, 1)
        prof_ref[it : it + 1, :] = moved[:, 0:tiles]

    @pl.when(is_root)
    def _():
        for i in range(answers):
            answer_copy(i).wait_send()


def finish_kernel(field, prof, field_out, prof_out, buffer, sems):
    halves = 2
    reads = [pltpu.make_async_copy(field.at[i], buffer.at[i], sems.at[i]) for i in range(halves)]
    writes = [pltpu.make_async_copy(buffer.at[i], field_out.at[i], sems.at[2 + i]) for i in range(halves)]
    for read in reads:
        read.start()
    prof_out[...] = prof[...]
    for read, write in zip(reads, writes):
        read.wait()
        write.start()
    for write in writes:
        write.wait()


def finish(field, prof):
    any_spec = pl.BlockSpec(memory_space=pl.ANY)
    vmem = pl.BlockSpec(memory_space=pltpu.VMEM)
    return pl.pallas_call(
        finish_kernel,
        out_shape=(
            jax.ShapeDtypeStruct(field.shape, F32),
            jax.ShapeDtypeStruct(prof.shape, F32),
        ),
        in_specs=[any_spec, vmem],
        out_specs=(any_spec, vmem),
        scratch_shapes=[pltpu.VMEM(field.shape, F32), pltpu.SemaphoreType.DMA((4,))],
        name="finish",
    )(field, prof)


def per_device(phase):
    n = lax.axis_size("rows")
    height, width = phase.shape
    tiles = width // LANES
    consts = [jnp.asarray(t) for t in tables()]
    stages = int(math.log2(n)) - 2
    chunks = len(PHASE_ENDS)
    dma = pltpu.SemaphoreType.DMA
    any_spec = pl.BlockSpec(memory_space=pl.ANY)
    results = pl.pallas_call(
        functools.partial(kernel, n, tiles),
        out_shape=(
            jax.ShapeDtypeStruct((2, height, width), F32),
            jax.ShapeDtypeStruct((ITERS, tiles), F32),
        ),
        in_specs=[any_spec] * 6,
        out_specs=(any_spec, pl.BlockSpec(memory_space=pltpu.VMEM)),
        scratch_shapes=[
            pltpu.VMEM((2, height, width), F32),
            *[pltpu.VMEM(c.shape, c.dtype) for c in consts[:4]],
            pltpu.VMEM(consts[4].shape, consts[4].dtype),
            pltpu.VMEM((tiles + 1, 2 * WIN, LANES), F32),
            pltpu.VMEM((ITERS, 2, tiles, WIN, LANES), F32),
            pltpu.VMEM((ITERS, 2, tiles, WIN, LANES), F32),
            pltpu.VMEM((2 * WIN, LANES), F32),
            pltpu.VMEM((2, height, width), F32),
            pltpu.VMEM((1, LANES), F32),
            pltpu.VMEM((n, 1, LANES), F32),
            pltpu.VMEM((1, LANES), F32),
            dma((6,)),
            dma((chunks,)),
            dma((chunks,)),
            dma((ITERS, chunks)),
            dma((ITERS, chunks)),
            dma((ITERS, chunks)),
            dma((ITERS, chunks)),
            dma((ROOTS,)),
            dma,
            dma((n // ROOTS - 1,)),
            dma,
            dma,
            pltpu.SemaphoreType.REGULAR((stages,)),
        ],
        compiler_params=pltpu.CompilerParams(
            collective_id=0, has_side_effects=True, vmem_limit_bytes=60 << 20
        ),
        name="goldstein",
    )(phase, *consts)
    return finish(*results)


def solution(mesh):
    return jax.shard_map(
        per_device,
        mesh=mesh,
        in_specs=(P(("groups", "rows"), None),),
        out_specs=(P(None, ("groups", "rows"), None), P("groups", None)),
        check_vma=False,
    )
```

```python
import functools
import math

import jax
import jax.numpy as jnp
import numpy as np
from jax import lax
from jax.experimental import pallas as pl
from jax.experimental.pallas import tpu as pltpu
from jax.sharding import PartitionSpec as P

ITERS = 3
EPS = 1e-06
WIN = 32
HALF = 16
LANES = 128
F32 = jnp.float32
BF16 = jnp.bfloat16
MESH = pl.DeviceIdType.MESH
ROOTS = 4

PHASE_ENDS = (7, 12, 16)
CHUNK_ENDS = ((6, 11, 16), (5, 10, 16), (4, 9, 16))


def hi_lo(table):
    high = table.astype(np.float32).astype(jnp.bfloat16)
    low = (table - high.astype(np.float64)).astype(np.float32).astype(jnp.bfloat16)
    return high, low


def tables():
    counter = np.arange(WIN)
    angles = 2.0 * math.pi / WIN * (counter[:, None] * counter[None, :] % WIN)
    cos, sin = np.cos(angles), np.sin(angles)
    ramp = 1.0 - np.abs(counter - 15.5) / 16.0

    def rows(real, imag):
        return np.concatenate([real[:HALF], imag[:HALF], real[HALF:], imag[HALF:]])

    forward = np.concatenate(
        [rows(cos.T, sin.T).T, rows(-sin.T, cos.T).T], axis=0
    )
    high, low = hi_lo(forward)
    row_in = np.concatenate([high, high, low], axis=1)
    scale = ramp[:, None] / WIN
    backward = rows(
        np.concatenate([cos, -sin], axis=1) * scale, np.concatenate([sin, cos], axis=1) * scale
    )
    high, low = hi_lo(backward)
    row_out = np.concatenate([high, high, low], axis=1)
    four = np.eye(LANES // WIN)
    c, s = np.kron(four, cos), np.kron(four, sin)
    high, low = hi_lo(np.block([[c, -s], [s, c]]))
    col_in = np.concatenate([high, high, low], axis=0)
    taper = np.tile(ramp, LANES // WIN)[None, :] / WIN
    high, low = hi_lo(np.block([[c * taper, s * taper], [-s * taper, c * taper]]))
    col_out = np.concatenate([high, high, low], axis=0)
    ones = np.kron(four, np.ones((WIN, WIN)))
    ones = np.concatenate([ones, ones], axis=0).astype(jnp.bfloat16)
    return [row_in, col_in, col_out, row_out, ones]


def split(x):
    high = x.astype(BF16)
    return high, (x - high.astype(F32)).astype(BF16)


def split_rows(x):
    high, low = split(x)
    return jnp.concatenate([high, low, high], axis=0)


def split_cols(x):
    high, low = split(x)
    return jnp.concatenate([high, low, high], axis=1)


def dot(a, b):
    return jnp.dot(a, b, preferred_element_type=F32)


def unit(phase):
    y = phase * 0.5
    t = y * y
    sine = -1.0 / 39916800.0
    for c in (1.0 / 362880.0, -1.0 / 5040.0, 1.0 / 120.0, -1.0 / 6.0, 1.0):
        sine = sine * t + c
    sine = sine * y
    cosine = 1.0 / 479001600.0
    for c in (-1.0 / 3628800.0, 1.0 / 40320.0, -1.0 / 720.0, 1.0 / 24.0, -0.5, 1.0):
        cosine = cosine * t + c
    return 1.0 - 2.0 * (sine * sine), 2.0 * (sine * cosine)


def to_lanes(tiles):
    return jnp.concatenate([tiles[j] for j in range(tiles.shape[0])], axis=1)


def to_tiles(wide):
    return jnp.stack(
        [wide[:, LANES * j : LANES * (j + 1)] for j in range(wide.shape[1] // LANES)]
    )


def kernel(
    n,
    tiles,
    phase_hbm,
    row_in_hbm,
    col_in_hbm,
    col_out_hbm,
    row_out_hbm,
    ones_hbm,
    out_ref,
    prof_ref,
    phase,
    row_in,
    col_in,
    col_out,
    row_out,
    ones,
    x,
    eo,
    rv,
    carry,
    pay,
    got,
    answer,
    load_sem,
    ph_send,
    ph_recv,
    up_send,
    up_recv,
    dn_send,
    dn_recv,
    pay_send,
    pay_recv,
    ans_send,
    ans_recv,
    relay,
):
    me = lax.axis_index("rows")
    has_above = me > 0
    has_below = me < n - 1

    def ring(offset):
        return {"rows": lax.rem(me + (offset + n), n)}

    def greet(sem, distance):
        for offset in (-distance, distance):
            pl.semaphore_signal(sem, inc=1, device_id=ring(offset), device_id_type=MESH)

    barrier = pltpu.get_barrier_semaphore()
    greet(barrier, 1)
    greet(barrier, 2)

    loads = [
        pltpu.make_async_copy(src, dst, load_sem.at[i])
        for i, (src, dst) in enumerate(
            [
                (phase_hbm, phase.at[0]),
                (row_in_hbm, row_in),
                (ones_hbm, ones),
                (col_in_hbm, col_in),
                (col_out_hbm, col_out),
                (row_out_hbm, row_out),
            ]
        )
    ]
    for load in loads:
        load.start()

    keep_below = jnp.where(has_below, 1.0, 0.0).astype(F32)

    @pl.when(jnp.logical_not(has_above))
    def _():
        rv[:, 0] = jnp.zeros(rv.shape[:1] + rv.shape[2:], F32)

    @pl.when(jnp.logical_not(has_below))
    def _():
        rv[:, 1] = jnp.zeros(rv.shape[:1] + rv.shape[2:], F32)
        phase[1] = jnp.zeros(phase.shape[1:], F32)

    x[tiles] = jnp.zeros(x.shape[1:], F32)
    loads[0].wait()
    pl.semaphore_wait(barrier, 4)

    stages = relay.shape[0]
    greet(relay.at[0], 2)

    def relay_step(s):
        if s < stages:
            pl.semaphore_wait(relay.at[s], 2)
            if s + 1 < stages:
                greet(relay.at[s + 1], 4 * 2 ** s)

    def phase_copy(c):
        first = PHASE_ENDS[c - 1] if c else 0
        cols = pl.ds(first * LANES, (PHASE_ENDS[c] - first) * LANES)
        return pltpu.make_async_remote_copy(
            src_ref=phase.at[0, :, cols],
            dst_ref=phase.at[1, :, cols],
            send_sem=ph_send.at[c],
            recv_sem=ph_recv.at[c],
            device_id={"rows": jnp.maximum(me - 1, 0)},
            device_id_type=MESH,
        )

    def span(it, c):
        ends = CHUNK_ENDS[it]
        return (ends[c - 1] if c else 0), ends[c]

    def up_copy(it, c):
        lo, hi = span(it, c)
        return pltpu.make_async_remote_copy(
            src_ref=eo.at[it, 0, pl.ds(lo, hi - lo)],
            dst_ref=rv.at[it, 1, pl.ds(lo, hi - lo)],
            send_sem=up_send.at[it, c],
            recv_sem=up_recv.at[it, c],
            device_id={"rows": jnp.maximum(me - 1, 0)},
            device_id_type=MESH,
        )

    def dn_copy(it, c):
        lo, hi = span(it, c)
        return pltpu.make_async_remote_copy(
            src_ref=eo.at[it, 1, pl.ds(lo, hi - lo)],
            dst_ref=rv.at[it, 0, pl.ds(lo, hi - lo)],
            send_sem=dn_send.at[it, c],
            recv_sem=dn_recv.at[it, c],
            device_id={"rows": jnp.minimum(me + 1, n - 1)},
            device_id_type=MESH,
        )

    @pl.when(has_above)
    def _():
        for c in range(len(PHASE_ENDS)):
            phase_copy(c).start()

    lane = lax.broadcasted_iota(jnp.int32, (1, 1, LANES), 2)

    def unit_tiles(row, lo, hi, scale=None):
        real, imag = unit(phase[row, :, lo * LANES : hi * LANES])
        if scale is not None:
            real, imag = real * scale, imag * scale
        return to_tiles(jnp.concatenate([real, imag], axis=0))

    x[0:tiles, 0:WIN] = unit_tiles(0, 0, tiles)
    for load in loads[1:]:
        load.wait()
    below_rows = lax.broadcasted_iota(jnp.int32, row_out.shape, 0) >= WIN
    row_out[...] = jnp.where(
        jnp.logical_and(below_rows, jnp.logical_not(has_below)),
        jnp.zeros(row_out.shape, BF16),
        row_out[...],
    )

    def arrive(it, c):
        if it == 0:
            lo, hi = (PHASE_ENDS[c - 1] if c else 0), PHASE_ENDS[c]

            @pl.when(has_above)
            def _():
                phase_copy(c).wait_send()

            @pl.when(has_below)
            def _():
                phase_copy(c).wait_recv()

            x[lo:hi, WIN:] = unit_tiles(1, lo, hi, keep_below)
            return hi
        lo, hi = span(it - 1, c)

        @pl.when(has_above)
        def _():
            up_copy(it - 1, c).wait_send()
            dn_copy(it - 1, c).wait_recv()

        @pl.when(has_below)
        def _():
            up_copy(it - 1, c).wait_recv()
            dn_copy(it - 1, c).wait_send()

        x[lo:hi] = jnp.concatenate(
            [eo[it - 1, 0, lo:hi] + rv[it - 1, 0, lo:hi], eo[it - 1, 1, lo:hi] + rv[it - 1, 1, lo:hi]],
            axis=1,
        )
        return hi

    def residues(it, lo, hi):
        field = x[lo : hi + 1]
        last_row = lax.broadcasted_iota(jnp.int32, (1, HALF, 1), 1) == HALF - 1

        def lower(a, b):
            return jnp.where(last_row, b[:, 0:1], pltpu.roll(a, HALF - 1, 1))

        def right(a):
            return pltpu.roll(jnp.where(lane == 0, a[1:], a[:-1]), LANES - 1, 2)

        ar, ai = field[:, 0:HALF], field[:, HALF:WIN]
        dr = lower(ar, field[:, WIN : WIN + HALF])
        di = lower(ai, field[:, WIN + HALF :])
        pr, pi = ar[:-1] - right(dr), ai[:-1] - right(di)
        qr, qi = right(ar) - dr[:-1], right(ai) - di[:-1]
        loop = pi * qr - pr * qi
        loop = loop * loop
        loop = loop[:, 0:8] + loop[:, 8:HALF]
        sums = jnp.sum(loop, axis=2, keepdims=True)
        lanes = lax.broadcasted_iota(jnp.int32, (8, LANES), 1)
        total = jnp.zeros((8, LANES), F32)
        for j in range(hi - lo):
            total = jnp.where(lanes == it * tiles + lo + j, sums[j], total)
        return total

    def windows(it, lo, hi):
        count = hi - lo
        field = x[lo : hi + 1]
        y = to_tiles(dot(row_in[...], split_rows(to_lanes(field))))
        square = field * field
        square = sum(square[:, 8 * i : 8 * i + 8] for i in range(8))

        def both(tall):
            odd = pltpu.roll(jnp.where(lane < HALF, tall[1:], tall[:-1]), LANES - HALF, 2)
            return jnp.concatenate([tall[:-1], odd], axis=0)

        high, low = split(both(square).reshape(2 * count * 8, LANES))
        mean = dot(jnp.concatenate([high, low], axis=1), ones[...])
        mean = jnp.sum(mean.reshape(2 * count, 8, LANES), axis=1, keepdims=True)
        inverse = 1.0 / (mean + EPS)

        y = both(y)
        y = jnp.concatenate([y[:, 0:WIN], y[:, WIN:]], axis=2).reshape(2 * count * WIN, 2 * LANES)
        s = dot(split_cols(y), col_in[...]).reshape(2 * count, WIN, 2 * LANES)
        sr, si = s[:, :, 0:LANES], s[:, :, LANES:]
        gain = lax.rsqrt(lax.rsqrt((sr * sr + si * si) * inverse))
        s = jnp.concatenate([sr * gain, si * gain], axis=2).reshape(2 * count * WIN, 2 * LANES)
        s = dot(split_cols(s), col_out[...]).reshape(2 * count, WIN, 2 * LANES)
        s = jnp.concatenate([s[:, :, 0:LANES], s[:, :, LANES:]], axis=1)
        moved = pltpu.roll(s[count:], HALF, 2)
        if lo == 0:
            before = jnp.zeros((1, 2 * WIN, LANES), F32)
        else:
            before = carry[...][None]
        if hi < tiles:
            carry[...] = moved[count - 1]
        before = jnp.concatenate([before, moved[:-1]], axis=0)
        s = s[:count] + jnp.where(lane < HALF, before, moved)
        result = to_tiles(dot(row_out[...], split_rows(to_lanes(s))))
        eo[it, 0, lo:hi] = result[:, 0:WIN]
        eo[it, 1, lo:hi] = result[:, WIN:]

    def pay_copy(root):
        return pltpu.make_async_remote_copy(
            src_ref=pay,
            dst_ref=got.at[lax.rem(me - root + n, n)],
            send_sem=pay_send.at[root],
            recv_sem=pay_recv,
            device_id={"rows": root},
            device_id_type=MESH,
        )

    def answer_copy(i):
        return pltpu.make_async_remote_copy(
            src_ref=answer,
            dst_ref=answer,
            send_sem=ans_send.at[i],
            recv_sem=ans_recv,
            device_id={"rows": jnp.minimum(me + ROOTS * (i + 1), n - 1)},
            device_id_type=MESH,
        )

    chunks = len(PHASE_ENDS)
    payload = jnp.zeros((8, LANES), F32)
    relay_step(0)
    for it in range(ITERS - 1):
        for c in range(chunks):
            lo, hi = span(it, c)
            arrive(it, c)
            if c == 0 and it == 0:
                relay_step(1)
            windows(it, lo, hi)

            @pl.when(has_above)
            def _():
                up_copy(it, c).start()

            @pl.when(has_below)
            def _():
                dn_copy(it, c).start()

        payload = payload + residues(it, 0, tiles)
        if it == 0:
            relay_step(2)

    last = ITERS - 1
    for c in range(chunks):
        arrive(last, c)
        payload = payload + residues(last, *span(last, c))
    pay[...] = jnp.sum(payload, axis=0, keepdims=True)
    for s in range(3, stages):
        relay_step(s)
    for root in range(ROOTS):

        @pl.when(me != root)
        def _():
            pay_copy(root).start()

    for c in range(chunks):
        windows(last, *span(last, c))

        @pl.when(has_below)
        def _():
            dn_copy(last, c).start()

    for c in range(chunks):
        lo, hi = span(last, c)

        @pl.when(has_above)
        def _():
            dn_copy(last, c).wait_recv()

        @pl.when(has_below)
        def _():
            dn_copy(last, c).wait_send()

        final = to_lanes(eo[last, 0, lo:hi] + rv[last, 0, lo:hi])
        out_ref[0, :, lo * LANES : hi * LANES] = final[0:HALF]
        out_ref[1, :, lo * LANES : hi * LANES] = final[HALF:]
    for root in range(ROOTS):

        @pl.when(me != root)
        def _():
            pay_copy(root).wait_send()

    is_root = me < ROOTS
    answers = ans_send.shape[0]

    @pl.when(is_root)
    def _():
        others = got.at[pl.ds(1, n - 1)]
        pltpu.make_async_remote_copy(
            src_ref=others,
            dst_ref=others,
            send_sem=pay_send.at[0],
            recv_sem=pay_recv,
            device_id=ring(1),
            device_id_type=MESH,
        ).wait_recv()
        total = pay[...] + jnp.sum(got[1:n], axis=0)
        answer[...] = total * (1.0 / (n * HALF * LANES))
        for i in range(answers):
            answer_copy(i).start()

    @pl.when(jnp.logical_not(is_root))
    def _():
        answer_copy(0).wait_recv()

    for it in range(ITERS):
        moved = answer[...] if it == 0 else pltpu.roll(answer[...], LANES - it * tiles, 1)
        prof_ref[it : it + 1, :] = moved[:, 0:tiles]

    @pl.when(is_root)
    def _():
        for i in range(answers):
            answer_copy(i).wait_send()


def per_device(phase):
    n = lax.axis_size("rows")
    height, width = phase.shape
    tiles = width // LANES
    consts = [jnp.asarray(t) for t in tables()]
    stages = int(math.log2(n)) - 2
    chunks = len(PHASE_ENDS)
    dma = pltpu.SemaphoreType.DMA
    any_spec = pl.BlockSpec(memory_space=pl.ANY)
    return pl.pallas_call(
        functools.partial(kernel, n, tiles),
        out_shape=(
            pltpu.VMEM((2, height, width), F32),
            pltpu.VMEM((ITERS, tiles), F32),
        ),
        in_specs=[any_spec] * 6,
        out_specs=(pl.BlockSpec(memory_space=pltpu.VMEM), pl.BlockSpec(memory_space=pltpu.VMEM)),
        scratch_shapes=[
            pltpu.VMEM((2, height, width), F32),
            *[pltpu.VMEM(c.shape, c.dtype) for c in consts[:4]],
            pltpu.VMEM(consts[4].shape, consts[4].dtype),
            pltpu.VMEM((tiles + 1, 2 * WIN, LANES), F32),
            pltpu.VMEM((ITERS, 2, tiles, WIN, LANES), F32),
            pltpu.VMEM((ITERS, 2, tiles, WIN, LANES), F32),
            pltpu.VMEM((2 * WIN, LANES), F32),
            pltpu.VMEM((1, LANES), F32),
            pltpu.VMEM((n, 1, LANES), F32),
            pltpu.VMEM((1, LANES), F32),
            dma((6,)),
            dma((chunks,)),
            dma((chunks,)),
            dma((ITERS, chunks)),
            dma((ITERS, chunks)),
            dma((ITERS, chunks)),
            dma((ITERS, chunks)),
            dma((ROOTS,)),
            dma,
            dma((n // ROOTS - 1,)),
            dma,
            pltpu.SemaphoreType.REGULAR((stages,)),
        ],
        compiler_params=pltpu.CompilerParams(
            collective_id=0, has_side_effects=True, vmem_limit_bytes=60 << 20
        ),
        name="goldstein",
    )(phase, *consts)


def solution(mesh):
    return jax.shard_map(
        per_device,
        mesh=mesh,
        in_specs=(P(("groups", "rows"), None),),
        out_specs=(P(None, ("groups", "rows"), None), P("groups", None)),
        check_vma=False,
    )
```

```python
import functools
import math

import jax
import jax.numpy as jnp
import numpy as np
from jax import lax
from jax.experimental import pallas as pl
from jax.experimental.pallas import tpu as pltpu
from jax.sharding import PartitionSpec as P

ITERS = 3
EPS = 1e-06
WIN = 32
HALF = 16
LANES = 128
F32 = jnp.float32
BF16 = jnp.bfloat16
MESH = pl.DeviceIdType.MESH
ROOTS = 4

PHASE_ENDS = (7, 12, 16)
CHUNK_ENDS = ((6, 11, 16), (5, 10, 16), (4, 9, 16))


def hi_lo(table):
    high = table.astype(np.float32).astype(jnp.bfloat16)
    low = (table - high.astype(np.float64)).astype(np.float32).astype(jnp.bfloat16)
    return high, low


def tables():
    counter = np.arange(WIN)
    angles = 2.0 * math.pi / WIN * (counter[:, None] * counter[None, :] % WIN)
    cos, sin = np.cos(angles), np.sin(angles)
    ramp = 1.0 - np.abs(counter - 15.5) / 16.0

    def rows(real, imag):
        return np.concatenate([real[:HALF], imag[:HALF], real[HALF:], imag[HALF:]])

    forward = np.concatenate(
        [rows(cos.T, sin.T).T, rows(-sin.T, cos.T).T], axis=0
    )
    high, low = hi_lo(forward)
    row_in = np.concatenate([high, high, low], axis=1)
    scale = ramp[:, None] / WIN
    backward = rows(
        np.concatenate([cos, -sin], axis=1) * scale, np.concatenate([sin, cos], axis=1) * scale
    )
    high, low = hi_lo(backward)
    row_out = np.concatenate([high, high, low], axis=1)
    four = np.eye(LANES // WIN)
    c, s = np.kron(four, cos), np.kron(four, sin)
    high, low = hi_lo(np.block([[c, -s], [s, c]]))
    col_in = np.concatenate([high, high, low], axis=0)
    taper = np.tile(ramp, LANES // WIN)[None, :] / WIN
    high, low = hi_lo(np.block([[c * taper, s * taper], [-s * taper, c * taper]]))
    col_out = np.concatenate([high, high, low], axis=0)
    ones = np.kron(four, np.ones((WIN, WIN)))
    ones = np.concatenate([ones, ones], axis=0).astype(jnp.bfloat16)
    return [row_in, col_in, col_out, row_out, ones]


def split(x):
    high = x.astype(BF16)
    return high, (x - high.astype(F32)).astype(BF16)


def split_rows(x):
    high, low = split(x)
    return jnp.concatenate([high, low, high], axis=0)


def split_cols(x):
    high, low = split(x)
    return jnp.concatenate([high, low, high], axis=1)


def dot(a, b):
    return jnp.dot(a, b, preferred_element_type=F32)


def unit(phase):
    y = phase * 0.5
    t = y * y
    sine = -1.0 / 39916800.0
    for c in (1.0 / 362880.0, -1.0 / 5040.0, 1.0 / 120.0, -1.0 / 6.0, 1.0):
        sine = sine * t + c
    sine = sine * y
    cosine = 1.0 / 479001600.0
    for c in (-1.0 / 3628800.0, 1.0 / 40320.0, -1.0 / 720.0, 1.0 / 24.0, -0.5, 1.0):
        cosine = cosine * t + c
    return 1.0 - 2.0 * (sine * sine), 2.0 * (sine * cosine)


def to_lanes(tiles):
    return jnp.concatenate([tiles[j] for j in range(tiles.shape[0])], axis=1)


def to_tiles(wide):
    return jnp.stack(
        [wide[:, LANES * j : LANES * (j + 1)] for j in range(wide.shape[1] // LANES)]
    )


def kernel(
    n,
    tiles,
    phase_hbm,
    row_in_hbm,
    col_in_hbm,
    col_out_hbm,
    row_out_hbm,
    ones_hbm,
    out_ref,
    prof_ref,
    phase,
    row_in,
    col_in,
    col_out,
    row_out,
    ones,
    x,
    eo,
    rv,
    carry,
    pay,
    got,
    answer,
    load_sem,
    ph_send,
    ph_recv,
    up_send,
    up_recv,
    dn_send,
    dn_recv,
    pay_send,
    pay_recv,
    ans_send,
    ans_recv,
    relay,
):
    me = lax.axis_index("rows")
    has_above = me > 0
    has_below = me < n - 1

    def ring(offset):
        return {"rows": lax.rem(me + (offset + n), n)}

    def greet(sem, distance):
        for offset in (-distance, distance):
            pl.semaphore_signal(sem, inc=1, device_id=ring(offset), device_id_type=MESH)

    barrier = pltpu.get_barrier_semaphore()
    greet(barrier, 1)
    greet(barrier, 2)

    loads = [
        pltpu.make_async_copy(src, dst, load_sem.at[i])
        for i, (src, dst) in enumerate(
            [
                (phase_hbm, phase.at[0]),
                (row_in_hbm, row_in),
                (ones_hbm, ones),
                (col_in_hbm, col_in),
                (col_out_hbm, col_out),
                (row_out_hbm, row_out),
            ]
        )
    ]
    for load in loads:
        load.start()

    keep_below = jnp.where(has_below, 1.0, 0.0).astype(F32)

    @pl.when(jnp.logical_not(has_above))
    def _():
        rv[:, 0] = jnp.zeros(rv.shape[:1] + rv.shape[2:], F32)

    @pl.when(jnp.logical_not(has_below))
    def _():
        rv[:, 1] = jnp.zeros(rv.shape[:1] + rv.shape[2:], F32)
        phase[1] = jnp.zeros(phase.shape[1:], F32)

    x[tiles] = jnp.zeros(x.shape[1:], F32)
    loads[0].wait()
    pl.semaphore_wait(barrier, 4)

    stages = relay.shape[0]
    greet(relay.at[0], 2)

    def relay_step(s):
        if s < stages:
            pl.semaphore_wait(relay.at[s], 2)
            if s + 1 < stages:
                greet(relay.at[s + 1], 4 * 2 ** s)

    def phase_copy(c):
        first = PHASE_ENDS[c - 1] if c else 0
        cols = pl.ds(first * LANES, (PHASE_ENDS[c] - first) * LANES)
        return pltpu.make_async_remote_copy(
            src_ref=phase.at[0, :, cols],
            dst_ref=phase.at[1, :, cols],
            send_sem=ph_send.at[c],
            recv_sem=ph_recv.at[c],
            device_id={"rows": jnp.maximum(me - 1, 0)},
            device_id_type=MESH,
        )

    def span(it, c):
        ends = CHUNK_ENDS[it]
        return (ends[c - 1] if c else 0), ends[c]

    def up_copy(it, c):
        lo, hi = span(it, c)
        return pltpu.make_async_remote_copy(
            src_ref=eo.at[it, 0, pl.ds(lo, hi - lo)],
            dst_ref=rv.at[it, 1, pl.ds(lo, hi - lo)],
            send_sem=up_send.at[it, c],
            recv_sem=up_recv.at[it, c],
            device_id={"rows": jnp.maximum(me - 1, 0)},
            device_id_type=MESH,
        )

    def dn_copy(it, c):
        lo, hi = span(it, c)
        return pltpu.make_async_remote_copy(
            src_ref=eo.at[it, 1, pl.ds(lo, hi - lo)],
            dst_ref=rv.at[it, 0, pl.ds(lo, hi - lo)],
            send_sem=dn_send.at[it, c],
            recv_sem=dn_recv.at[it, c],
            device_id={"rows": jnp.minimum(me + 1, n - 1)},
            device_id_type=MESH,
        )

    @pl.when(has_above)
    def _():
        for c in range(len(PHASE_ENDS)):
            phase_copy(c).start()

    lane = lax.broadcasted_iota(jnp.int32, (1, 1, LANES), 2)

    def unit_tiles(row, lo, hi, scale=None):
        real, imag = unit(phase[row, :, lo * LANES : hi * LANES])
        if scale is not None:
            real, imag = real * scale, imag * scale
        return to_tiles(jnp.concatenate([real, imag], axis=0))

    x[0:tiles, 0:WIN] = unit_tiles(0, 0, tiles)
    for load in loads[1:]:
        load.wait()
    below_rows = lax.broadcasted_iota(jnp.int32, row_out.shape, 0) >= WIN
    row_out[...] = jnp.where(
        jnp.logical_and(below_rows, jnp.logical_not(has_below)),
        jnp.zeros(row_out.shape, BF16),
        row_out[...],
    )

    def arrive(it, c):
        if it == 0:
            lo, hi = (PHASE_ENDS[c - 1] if c else 0), PHASE_ENDS[c]

            @pl.when(has_below)
            def _():
                phase_copy(c).wait_recv()

            x[lo:hi, WIN:] = unit_tiles(1, lo, hi, keep_below)
            return hi
        lo, hi = span(it - 1, c)

        @pl.when(has_above)
        def _():
            dn_copy(it - 1, c).wait_recv()

        @pl.when(has_below)
        def _():
            up_copy(it - 1, c).wait_recv()

        x[lo:hi] = jnp.concatenate(
            [eo[it - 1, 0, lo:hi] + rv[it - 1, 0, lo:hi], eo[it - 1, 1, lo:hi] + rv[it - 1, 1, lo:hi]],
            axis=1,
        )
        return hi

    def residues(it, lo, hi):
        field = x[lo : hi + 1]
        last_row = lax.broadcasted_iota(jnp.int32, (1, HALF, 1), 1) == HALF - 1

        def lower(a, b):
            return jnp.where(last_row, b[:, 0:1], pltpu.roll(a, HALF - 1, 1))

        def right(a):
            return pltpu.roll(jnp.where(lane == 0, a[1:], a[:-1]), LANES - 1, 2)

        ar, ai = field[:, 0:HALF], field[:, HALF:WIN]
        dr = lower(ar, field[:, WIN : WIN + HALF])
        di = lower(ai, field[:, WIN + HALF :])
        pr, pi = ar[:-1] - right(dr), ai[:-1] - right(di)
        qr, qi = right(ar) - dr[:-1], right(ai) - di[:-1]
        loop = pi * qr - pr * qi
        loop = loop * loop
        loop = loop[:, 0:8] + loop[:, 8:HALF]
        sums = jnp.sum(loop, axis=2, keepdims=True)
        lanes = lax.broadcasted_iota(jnp.int32, (8, LANES), 1)
        total = jnp.zeros((8, LANES), F32)
        for j in range(hi - lo):
            total = jnp.where(lanes == it * tiles + lo + j, sums[j], total)
        return total

    def windows(it, lo, hi):
        count = hi - lo
        field = x[lo : hi + 1]
        y = to_tiles(dot(row_in[...], split_rows(to_lanes(field))))
        square = field * field
        square = sum(square[:, 8 * i : 8 * i + 8] for i in range(8))

        def both(tall):
            odd = pltpu.roll(jnp.where(lane < HALF, tall[1:], tall[:-1]), LANES - HALF, 2)
            return jnp.concatenate([tall[:-1], odd], axis=0)

        high, low = split(both(square).reshape(2 * count * 8, LANES))
        mean = dot(jnp.concatenate([high, low], axis=1), ones[...])
        mean = jnp.sum(mean.reshape(2 * count, 8, LANES), axis=1, keepdims=True)
        inverse = 1.0 / (mean + EPS)

        y = both(y)
        y = jnp.concatenate([y[:, 0:WIN], y[:, WIN:]], axis=2).reshape(2 * count * WIN, 2 * LANES)
        s = dot(split_cols(y), col_in[...]).reshape(2 * count, WIN, 2 * LANES)
        sr, si = s[:, :, 0:LANES], s[:, :, LANES:]
        gain = lax.rsqrt(lax.rsqrt((sr * sr + si * si) * inverse))
        s = jnp.concatenate([sr * gain, si * gain], axis=2).reshape(2 * count * WIN, 2 * LANES)
        s = dot(split_cols(s), col_out[...]).reshape(2 * count, WIN, 2 * LANES)
        s = jnp.concatenate([s[:, :, 0:LANES], s[:, :, LANES:]], axis=1)
        moved = pltpu.roll(s[count:], HALF, 2)
        if lo == 0:
            before = jnp.zeros((1, 2 * WIN, LANES), F32)
        else:
            before = carry[...][None]
        if hi < tiles:
            carry[...] = moved[count - 1]
        before = jnp.concatenate([before, moved[:-1]], axis=0)
        s = s[:count] + jnp.where(lane < HALF, before, moved)
        result = to_tiles(dot(row_out[...], split_rows(to_lanes(s))))
        eo[it, 0, lo:hi] = result[:, 0:WIN]
        eo[it, 1, lo:hi] = result[:, WIN:]

    def pay_copy(root):
        return pltpu.make_async_remote_copy(
            src_ref=pay,
            dst_ref=got.at[lax.rem(me - root + n, n)],
            send_sem=pay_send.at[root],
            recv_sem=pay_recv,
            device_id={"rows": root},
            device_id_type=MESH,
        )

    def answer_copy(i):
        return pltpu.make_async_remote_copy(
            src_ref=answer,
            dst_ref=answer,
            send_sem=ans_send.at[i],
            recv_sem=ans_recv,
            device_id={"rows": jnp.minimum(me + ROOTS * (i + 1), n - 1)},
            device_id_type=MESH,
        )

    chunks = len(PHASE_ENDS)
    payload = jnp.zeros((8, LANES), F32)
    relay_step(0)
    for it in range(ITERS - 1):
        for c in range(chunks):
            lo, hi = span(it, c)
            arrive(it, c)
            if it == 1 and c == 0:
                relay_step(2)
            windows(it, lo, hi)

            @pl.when(has_above)
            def _():
                up_copy(it, c).start()

            @pl.when(has_below)
            def _():
                dn_copy(it, c).start()

            if it == 0 and c == 0:
                relay_step(1)
        payload = payload + residues(it, 0, tiles)

    last = ITERS - 1
    for c in range(chunks):
        if c == chunks - 1:
            for s in range(3, stages):
                relay_step(s)
        arrive(last, c)
        payload = payload + residues(last, *span(last, c))
    pay[...] = jnp.sum(payload, axis=0, keepdims=True)
    for root in range(ROOTS):

        @pl.when(me != root)
        def _():
            pay_copy(root).start()

    for c in range(chunks):
        windows(last, *span(last, c))

        @pl.when(has_below)
        def _():
            dn_copy(last, c).start()

    for c in range(chunks):
        lo, hi = span(last, c)

        @pl.when(has_above)
        def _():
            dn_copy(last, c).wait_recv()

        final = to_lanes(eo[last, 0, lo:hi] + rv[last, 0, lo:hi])
        out_ref[0, :, lo * LANES : hi * LANES] = final[0:HALF]
        out_ref[1, :, lo * LANES : hi * LANES] = final[HALF:]
    @pl.when(has_above)
    def _():
        for c in range(chunks):
            phase_copy(c).wait_send()
            for it in range(last):
                up_copy(it, c).wait_send()

    @pl.when(has_below)
    def _():
        for it in range(ITERS):
            for c in range(chunks):
                dn_copy(it, c).wait_send()

    for root in range(ROOTS):

        @pl.when(me != root)
        def _():
            pay_copy(root).wait_send()

    is_root = me < ROOTS
    answers = ans_send.shape[0]

    @pl.when(is_root)
    def _():
        others = got.at[pl.ds(1, n - 1)]
        pltpu.make_async_remote_copy(
            src_ref=others,
            dst_ref=others,
            send_sem=pay_send.at[0],
            recv_sem=pay_recv,
            device_id=ring(1),
            device_id_type=MESH,
        ).wait_recv()
        total = pay[...] + jnp.sum(got[1:n], axis=0)
        answer[...] = total * (1.0 / (n * HALF * LANES))
        for i in range(answers):
            answer_copy(i).start()

    @pl.when(jnp.logical_not(is_root))
    def _():
        answer_copy(0).wait_recv()

    for it in range(ITERS):
        moved = answer[...] if it == 0 else pltpu.roll(answer[...], LANES - it * tiles, 1)
        prof_ref[it : it + 1, :] = moved[:, 0:tiles]

    @pl.when(is_root)
    def _():
        for i in range(answers):
            answer_copy(i).wait_send()


def finish_kernel(field, prof, field_out, prof_out, sems):
    copies = [
        pltpu.make_async_copy(field, field_out, sems.at[0]),
        pltpu.make_async_copy(prof, prof_out, sems.at[1]),
    ]
    for copy in copies:
        copy.start()
    for copy in copies:
        copy.wait()


def finish(field, prof):
    any_spec = pl.BlockSpec(memory_space=pl.ANY)
    vmem = pl.BlockSpec(memory_space=pltpu.VMEM)
    return pl.pallas_call(
        finish_kernel,
        out_shape=(
            jax.ShapeDtypeStruct(field.shape, F32),
            jax.ShapeDtypeStruct(prof.shape, F32),
        ),
        in_specs=[vmem, vmem],
        out_specs=(any_spec, any_spec),
        scratch_shapes=[pltpu.SemaphoreType.DMA((2,))],
        name="finish",
    )(field, prof)


def per_device(phase):
    n = lax.axis_size("rows")
    height, width = phase.shape
    tiles = width // LANES
    consts = [jnp.asarray(t) for t in tables()]
    stages = int(math.log2(n)) - 2
    chunks = len(PHASE_ENDS)
    dma = pltpu.SemaphoreType.DMA
    any_spec = pl.BlockSpec(memory_space=pl.ANY)
    results = pl.pallas_call(
        functools.partial(kernel, n, tiles),
        out_shape=(
            pltpu.VMEM((2, height, width), F32),
            pltpu.VMEM((ITERS, tiles), F32),
        ),
        in_specs=[any_spec] * 6,
        out_specs=(pl.BlockSpec(memory_space=pltpu.VMEM), pl.BlockSpec(memory_space=pltpu.VMEM)),
        scratch_shapes=[
            pltpu.VMEM((2, height, width), F32),
            *[pltpu.VMEM(c.shape, c.dtype) for c in consts[:4]],
            pltpu.VMEM(consts[4].shape, consts[4].dtype),
            pltpu.VMEM((tiles + 1, 2 * WIN, LANES), F32),
            pltpu.VMEM((ITERS, 2, tiles, WIN, LANES), F32),
            pltpu.VMEM((ITERS, 2, tiles, WIN, LANES), F32),
            pltpu.VMEM((2 * WIN, LANES), F32),
            pltpu.VMEM((1, LANES), F32),
            pltpu.VMEM((n, 1, LANES), F32),
            pltpu.VMEM((1, LANES), F32),
            dma((6,)),
            dma((chunks,)),
            dma((chunks,)),
            dma((ITERS, chunks)),
            dma((ITERS, chunks)),
            dma((ITERS, chunks)),
            dma((ITERS, chunks)),
            dma((ROOTS,)),
            dma,
            dma((n // ROOTS - 1,)),
            dma,
            pltpu.SemaphoreType.REGULAR((stages,)),
        ],
        compiler_params=pltpu.CompilerParams(
            collective_id=0, has_side_effects=True, vmem_limit_bytes=60 << 20
        ),
        name="goldstein",
    )(phase, *consts)
    return finish(*[pltpu.with_memory_space_constraint(r, pltpu.VMEM) for r in results])


def solution(mesh):
    return jax.shard_map(
        per_device,
        mesh=mesh,
        in_specs=(P(("groups", "rows"), None),),
        out_specs=(P(None, ("groups", "rows"), None), P("groups", None)),
        check_vma=False,
    )
```

```python
import functools
import math

import jax
import jax.numpy as jnp
import numpy as np
from jax import lax
from jax.experimental import pallas as pl
from jax.experimental.pallas import tpu as pltpu
from jax.sharding import PartitionSpec as P

ITERS = 3
EPS = 1e-06
WIN = 32
HALF = 16
LANES = 128
F32 = jnp.float32
BF16 = jnp.bfloat16
MESH = pl.DeviceIdType.MESH
ROOTS = 8
TELLERS = 4

PHASE_ENDS = (7, 12, 16)
CHUNK_ENDS = ((6, 11, 16), (5, 10, 16), (4, 9, 16))


def hi_lo(table):
    high = table.astype(np.float32).astype(jnp.bfloat16)
    low = (table - high.astype(np.float64)).astype(np.float32).astype(jnp.bfloat16)
    return high, low


def tables():
    counter = np.arange(WIN)
    angles = 2.0 * math.pi / WIN * (counter[:, None] * counter[None, :] % WIN)
    cos, sin = np.cos(angles), np.sin(angles)
    ramp = 1.0 - np.abs(counter - 15.5) / 16.0

    def rows(real, imag):
        return np.concatenate([real[:HALF], imag[:HALF], real[HALF:], imag[HALF:]])

    forward = np.concatenate(
        [rows(cos.T, sin.T).T, rows(-sin.T, cos.T).T], axis=0
    )
    high, low = hi_lo(forward)
    row_in = np.concatenate([high, high, low], axis=1)
    scale = ramp[:, None] / WIN
    backward = rows(
        np.concatenate([cos, -sin], axis=1) * scale, np.concatenate([sin, cos], axis=1) * scale
    )
    high, low = hi_lo(backward)
    row_out = np.concatenate([high, high, low], axis=1)
    four = np.eye(LANES // WIN)
    c, s = np.kron(four, cos), np.kron(four, sin)
    high, low = hi_lo(np.block([[c, -s], [s, c]]))
    col_in = np.concatenate([high, high, low], axis=0)
    taper = np.tile(ramp, LANES // WIN)[None, :] / WIN
    high, low = hi_lo(np.block([[c * taper, s * taper], [-s * taper, c * taper]]))
    col_out = np.concatenate([high, high, low], axis=0)
    ones = np.kron(four, np.ones((WIN, WIN)))
    ones = np.concatenate([ones, ones], axis=0).astype(jnp.bfloat16)
    return [row_in, col_in, col_out, row_out, ones]


def split(x):
    high = x.astype(BF16)
    return high, (x - high.astype(F32)).astype(BF16)


def split_rows(x):
    high, low = split(x)
    return jnp.concatenate([high, low, high], axis=0)


def split_cols(x):
    high, low = split(x)
    return jnp.concatenate([high, low, high], axis=1)


def dot(a, b):
    return jnp.dot(a, b, preferred_element_type=F32)


def unit(phase):
    y = phase * 0.5
    t = y * y
    sine = -1.0 / 39916800.0
    for c in (1.0 / 362880.0, -1.0 / 5040.0, 1.0 / 120.0, -1.0 / 6.0, 1.0):
        sine = sine * t + c
    sine = sine * y
    cosine = 1.0 / 479001600.0
    for c in (-1.0 / 3628800.0, 1.0 / 40320.0, -1.0 / 720.0, 1.0 / 24.0, -0.5, 1.0):
        cosine = cosine * t + c
    return 1.0 - 2.0 * (sine * sine), 2.0 * (sine * cosine)


def to_lanes(tiles):
    return jnp.concatenate([tiles[j] for j in range(tiles.shape[0])], axis=1)


def to_tiles(wide):
    return jnp.stack(
        [wide[:, LANES * j : LANES * (j + 1)] for j in range(wide.shape[1] // LANES)]
    )


def kernel(
    n,
    tiles,
    phase_hbm,
    row_in_hbm,
    col_in_hbm,
    col_out_hbm,
    row_out_hbm,
    ones_hbm,
    out_ref,
    prof_ref,
    phase,
    row_in,
    col_in,
    col_out,
    row_out,
    ones,
    x,
    eo,
    rv,
    carry,
    pay,
    got,
    answer,
    load_sem,
    ph_send,
    ph_recv,
    up_send,
    up_recv,
    dn_send,
    dn_recv,
    pay_send,
    pay_recv,
    ans_send,
    ans_recv,
    relay,
):
    me = lax.axis_index("rows")
    has_above = me > 0
    has_below = me < n - 1

    def ring(offset):
        return {"rows": lax.rem(me + (offset + n), n)}

    def greet(sem, distance):
        for offset in (-distance, distance):
            pl.semaphore_signal(sem, inc=1, device_id=ring(offset), device_id_type=MESH)

    barrier = pltpu.get_barrier_semaphore()
    greet(barrier, 1)
    greet(barrier, 2)

    loads = [
        pltpu.make_async_copy(src, dst, load_sem.at[i])
        for i, (src, dst) in enumerate(
            [
                (phase_hbm, phase.at[0]),
                (row_in_hbm, row_in),
                (ones_hbm, ones),
                (col_in_hbm, col_in),
                (col_out_hbm, col_out),
                (row_out_hbm, row_out),
            ]
        )
    ]
    for load in loads:
        load.start()

    keep_below = jnp.where(has_below, 1.0, 0.0).astype(F32)

    @pl.when(jnp.logical_not(has_above))
    def _():
        rv[:, 0] = jnp.zeros(rv.shape[:1] + rv.shape[2:], F32)

    @pl.when(jnp.logical_not(has_below))
    def _():
        rv[:, 1] = jnp.zeros(rv.shape[:1] + rv.shape[2:], F32)
        phase[1] = jnp.zeros(phase.shape[1:], F32)

    x[tiles] = jnp.zeros(x.shape[1:], F32)
    loads[0].wait()
    pl.semaphore_wait(barrier, 4)

    stages = relay.shape[0]
    greet(relay.at[0], 2)

    def relay_step(s):
        if s < stages:
            pl.semaphore_wait(relay.at[s], 2)
            if s + 1 < stages:
                greet(relay.at[s + 1], 4 * 2 ** s)

    def phase_copy(c):
        first = PHASE_ENDS[c - 1] if c else 0
        cols = pl.ds(first * LANES, (PHASE_ENDS[c] - first) * LANES)
        return pltpu.make_async_remote_copy(
            src_ref=phase.at[0, :, cols],
            dst_ref=phase.at[1, :, cols],
            send_sem=ph_send,
            recv_sem=ph_recv.at[c],
            device_id={"rows": jnp.maximum(me - 1, 0)},
            device_id_type=MESH,
        )

    def span(it, c):
        ends = CHUNK_ENDS[it]
        return (ends[c - 1] if c else 0), ends[c]

    def up_copy(it, c):
        lo, hi = span(it, c)
        return pltpu.make_async_remote_copy(
            src_ref=eo.at[it, 0, pl.ds(lo, hi - lo)],
            dst_ref=rv.at[it, 1, pl.ds(lo, hi - lo)],
            send_sem=up_send,
            recv_sem=up_recv.at[it, c],
            device_id={"rows": jnp.maximum(me - 1, 0)},
            device_id_type=MESH,
        )

    def dn_copy(it, c):
        lo, hi = span(it, c)
        return pltpu.make_async_remote_copy(
            src_ref=eo.at[it, 1, pl.ds(lo, hi - lo)],
            dst_ref=rv.at[it, 0, pl.ds(lo, hi - lo)],
            send_sem=dn_send,
            recv_sem=dn_recv.at[it, c],
            device_id={"rows": jnp.minimum(me + 1, n - 1)},
            device_id_type=MESH,
        )

    @pl.when(has_above)
    def _():
        for c in range(len(PHASE_ENDS)):
            phase_copy(c).start()

    lane = lax.broadcasted_iota(jnp.int32, (1, 1, LANES), 2)

    def unit_tiles(row, lo, hi, scale=None):
        real, imag = unit(phase[row, :, lo * LANES : hi * LANES])
        if scale is not None:
            real, imag = real * scale, imag * scale
        return to_tiles(jnp.concatenate([real, imag], axis=0))

    x[0:tiles, 0:WIN] = unit_tiles(0, 0, tiles)
    for load in loads[1:]:
        load.wait()
    below_rows = lax.broadcasted_iota(jnp.int32, row_out.shape, 0) >= WIN
    row_out[...] = jnp.where(
        jnp.logical_and(below_rows, jnp.logical_not(has_below)),
        jnp.zeros(row_out.shape, BF16),
        row_out[...],
    )

    def arrive(it, c):
        if it == 0:
            lo, hi = (PHASE_ENDS[c - 1] if c else 0), PHASE_ENDS[c]

            @pl.when(has_below)
            def _():
                phase_copy(c).wait_recv()

            x[lo:hi, WIN:] = unit_tiles(1, lo, hi, keep_below)
            return hi
        lo, hi = span(it - 1, c)

        @pl.when(has_above)
        def _():
            dn_copy(it - 1, c).wait_recv()

        @pl.when(has_below)
        def _():
            up_copy(it - 1, c).wait_recv()

        x[lo:hi] = jnp.concatenate(
            [eo[it - 1, 0, lo:hi] + rv[it - 1, 0, lo:hi], eo[it - 1, 1, lo:hi] + rv[it - 1, 1, lo:hi]],
            axis=1,
        )
        return hi

    def residues(it, lo, hi):
        field = x[lo : hi + 1]
        last_row = lax.broadcasted_iota(jnp.int32, (1, HALF, 1), 1) == HALF - 1

        def lower(a, b):
            return jnp.where(last_row, b[:, 0:1], pltpu.roll(a, HALF - 1, 1))

        def right(a):
            return pltpu.roll(jnp.where(lane == 0, a[1:], a[:-1]), LANES - 1, 2)

        ar, ai = field[:, 0:HALF], field[:, HALF:WIN]
        dr = lower(ar, field[:, WIN : WIN + HALF])
        di = lower(ai, field[:, WIN + HALF :])
        pr, pi = ar[:-1] - right(dr), ai[:-1] - right(di)
        qr, qi = right(ar) - dr[:-1], right(ai) - di[:-1]
        loop = pi * qr - pr * qi
        loop = loop * loop
        loop = loop[:, 0:8] + loop[:, 8:HALF]
        sums = jnp.sum(loop, axis=2, keepdims=True)
        lanes = lax.broadcasted_iota(jnp.int32, (8, LANES), 1)
        total = jnp.zeros((8, LANES), F32)
        for j in range(hi - lo):
            total = jnp.where(lanes == it * tiles + lo + j, sums[j], total)
        return total

    def windows(it, lo, hi):
        count = hi - lo
        field = x[lo : hi + 1]
        y = to_tiles(dot(row_in[...], split_rows(to_lanes(field))))
        square = field * field
        square = sum(square[:, 8 * i : 8 * i + 8] for i in range(8))

        def both(tall):
            odd = pltpu.roll(jnp.where(lane < HALF, tall[1:], tall[:-1]), LANES - HALF, 2)
            return jnp.concatenate([tall[:-1], odd], axis=0)

        high, low = split(both(square).reshape(2 * count * 8, LANES))
        mean = dot(jnp.concatenate([high, low], axis=1), ones[...])
        mean = jnp.sum(mean.reshape(2 * count, 8, LANES), axis=1, keepdims=True)
        inverse = 1.0 / (mean + EPS)

        y = both(y)
        y = jnp.concatenate([y[:, 0:WIN], y[:, WIN:]], axis=2).reshape(2 * count * WIN, 2 * LANES)
        s = dot(split_cols(y), col_in[...]).reshape(2 * count, WIN, 2 * LANES)
        sr, si = s[:, :, 0:LANES], s[:, :, LANES:]
        gain = lax.rsqrt(lax.rsqrt((sr * sr + si * si) * inverse))
        s = jnp.concatenate([sr * gain, si * gain], axis=2).reshape(2 * count * WIN, 2 * LANES)
        s = dot(split_cols(s), col_out[...]).reshape(2 * count, WIN, 2 * LANES)
        s = jnp.concatenate([s[:, :, 0:LANES], s[:, :, LANES:]], axis=1)
        moved = pltpu.roll(s[count:], HALF, 2)
        if lo == 0:
            before = jnp.zeros((1, 2 * WIN, LANES), F32)
        else:
            before = carry[...][None]
        if hi < tiles:
            carry[...] = moved[count - 1]
        before = jnp.concatenate([before, moved[:-1]], axis=0)
        s = s[:count] + jnp.where(lane < HALF, before, moved)
        result = to_tiles(dot(row_out[...], split_rows(to_lanes(s))))
        eo[it, 0, lo:hi] = result[:, 0:WIN]
        eo[it, 1, lo:hi] = result[:, WIN:]

    def pay_copy(root):
        return pltpu.make_async_remote_copy(
            src_ref=pay,
            dst_ref=got.at[lax.rem(me - root + n, n)],
            send_sem=pay_send,
            recv_sem=pay_recv,
            device_id={"rows": root},
            device_id_type=MESH,
        )

    def answer_copy(i):
        return pltpu.make_async_remote_copy(
            src_ref=answer,
            dst_ref=answer,
            send_sem=ans_send,
            recv_sem=ans_recv,
            device_id={"rows": jnp.minimum(me + TELLERS * (i + 1), n - 1)},
            device_id_type=MESH,
        )

    chunks = len(PHASE_ENDS)
    payload = jnp.zeros((8, LANES), F32)
    relay_step(0)
    for it in range(ITERS - 1):
        for c in range(chunks):
            lo, hi = span(it, c)
            arrive(it, c)
            if it == 1 and c == 0:
                relay_step(2)
            windows(it, lo, hi)

            @pl.when(has_above)
            def _():
                up_copy(it, c).start()

            @pl.when(has_below)
            def _():
                dn_copy(it, c).start()

            if it == 0 and c == 0:
                relay_step(1)
        payload = payload + residues(it, 0, tiles)

    last = ITERS - 1
    for c in range(chunks):
        if c == chunks - 1:
            for s in range(3, stages):
                relay_step(s)
        arrive(last, c)
        payload = payload + residues(last, *span(last, c))
    pay[...] = jnp.sum(payload, axis=0, keepdims=True)
    for root in range(ROOTS):

        @pl.when(me != root)
        def _():
            pay_copy(root).start()

    for c in range(chunks):
        windows(last, *span(last, c))

        @pl.when(has_below)
        def _():
            dn_copy(last, c).start()

    for c in range(chunks):
        lo, hi = span(last, c)

        @pl.when(has_above)
        def _():
            dn_copy(last, c).wait_recv()

        final = to_lanes(eo[last, 0, lo:hi] + rv[last, 0, lo:hi])
        out_ref[0, :, lo * LANES : hi * LANES] = final[0:HALF]
        out_ref[1, :, lo * LANES : hi * LANES] = final[HALF:]
    def sent(ref, sem):
        pltpu.make_async_remote_copy(
            src_ref=ref,
            dst_ref=ref,
            send_sem=sem,
            recv_sem=pay_recv,
            device_id=ring(1),
            device_id_type=MESH,
        ).wait_send()

    @pl.when(has_above)
    def _():
        sent(phase.at[0], ph_send)
        sent(eo.at[pl.ds(0, last), 0], up_send)

    @pl.when(has_below)
    def _():
        sent(eo.at[pl.ds(0, ITERS), 1], dn_send)

    is_root = me < ROOTS
    is_teller = jnp.logical_and(is_root, me >= ROOTS - TELLERS)
    answers = (n - ROOTS) // TELLERS

    @pl.when(is_root)
    def _():
        sent(got.at[pl.ds(0, ROOTS - 1)], pay_send)
        others = got.at[pl.ds(1, n - 1)]
        pltpu.make_async_remote_copy(
            src_ref=others,
            dst_ref=others,
            send_sem=pay_send,
            recv_sem=pay_recv,
            device_id=ring(1),
            device_id_type=MESH,
        ).wait_recv()
        total = pay[...] + jnp.sum(got[1:n], axis=0)
        answer[...] = total * (1.0 / (n * HALF * LANES))

    @pl.when(is_teller)
    def _():
        for i in range(answers):
            answer_copy(i).start()

    @pl.when(jnp.logical_not(is_root))
    def _():
        sent(got.at[pl.ds(0, ROOTS)], pay_send)
        answer_copy(0).wait_recv()

    for it in range(ITERS):
        moved = answer[...] if it == 0 else pltpu.roll(answer[...], LANES - it * tiles, 1)
        prof_ref[it : it + 1, :] = moved[:, 0:tiles]

    @pl.when(is_teller)
    def _():
        sent(got.at[pl.ds(0, answers)], ans_send)


def finish_kernel(field, prof, field_out, prof_out, sems):
    copies = [
        pltpu.make_async_copy(field, field_out, sems.at[0]),
        pltpu.make_async_copy(prof, prof_out, sems.at[1]),
    ]
    for copy in copies:
        copy.start()
    for copy in copies:
        copy.wait()


def finish(field, prof):
    any_spec = pl.BlockSpec(memory_space=pl.ANY)
    vmem = pl.BlockSpec(memory_space=pltpu.VMEM)
    return pl.pallas_call(
        finish_kernel,
        out_shape=(
            jax.ShapeDtypeStruct(field.shape, F32),
            jax.ShapeDtypeStruct(prof.shape, F32),
        ),
        in_specs=[vmem, vmem],
        out_specs=(any_spec, any_spec),
        scratch_shapes=[pltpu.SemaphoreType.DMA((2,))],
        name="finish",
    )(field, prof)


def per_device(phase):
    n = lax.axis_size("rows")
    height, width = phase.shape
    tiles = width // LANES
    consts = [jnp.asarray(t) for t in tables()]
    stages = int(math.log2(n)) - 2
    chunks = len(PHASE_ENDS)
    dma = pltpu.SemaphoreType.DMA
    any_spec = pl.BlockSpec(memory_space=pl.ANY)
    results = pl.pallas_call(
        functools.partial(kernel, n, tiles),
        out_shape=(
            pltpu.VMEM((2, height, width), F32),
            pltpu.VMEM((ITERS, tiles), F32),
        ),
        in_specs=[any_spec] * 6,
        out_specs=(pl.BlockSpec(memory_space=pltpu.VMEM), pl.BlockSpec(memory_space=pltpu.VMEM)),
        scratch_shapes=[
            pltpu.VMEM((2, height, width), F32),
            *[pltpu.VMEM(c.shape, c.dtype) for c in consts[:4]],
            pltpu.VMEM(consts[4].shape, consts[4].dtype),
            pltpu.VMEM((tiles + 1, 2 * WIN, LANES), F32),
            pltpu.VMEM((ITERS, 2, tiles, WIN, LANES), F32),
            pltpu.VMEM((ITERS, 2, tiles, WIN, LANES), F32),
            pltpu.VMEM((2 * WIN, LANES), F32),
            pltpu.VMEM((1, LANES), F32),
            pltpu.VMEM((n, 1, LANES), F32),
            pltpu.VMEM((1, LANES), F32),
            dma((6,)),
            dma,
            dma((chunks,)),
            dma,
            dma((ITERS, chunks)),
            dma,
            dma((ITERS, chunks)),
            dma,
            dma,
            dma,
            dma,
            pltpu.SemaphoreType.REGULAR((stages,)),
        ],
        compiler_params=pltpu.CompilerParams(
            collective_id=0, has_side_effects=True, vmem_limit_bytes=60 << 20
        ),
        name="goldstein",
    )(phase, *consts)
    return finish(*[pltpu.with_memory_space_constraint(r, pltpu.VMEM) for r in results])


def solution(mesh):
    return jax.shard_map(
        per_device,
        mesh=mesh,
        in_specs=(P(("groups", "rows"), None),),
        out_specs=(P(None, ("groups", "rows"), None), P("groups", None)),
        check_vma=False,
    )
```

```python
import functools
import math

import jax
import jax.numpy as jnp
import numpy as np
from jax import lax
from jax.experimental import pallas as pl
from jax.experimental.pallas import tpu as pltpu
from jax.sharding import PartitionSpec as P

ITERS = 3
EPS = 1e-06
WIN = 32
HALF = 16
LANES = 128
F32 = jnp.float32
BF16 = jnp.bfloat16
MESH = pl.DeviceIdType.MESH
ROOTS = 8
TELLERS = 4

PHASE_ENDS = (7, 12, 16)
CHUNK_ENDS = ((6, 11, 16), (5, 10, 16), (4, 9, 16))


def hi_lo(table):
    high = table.astype(np.float32).astype(jnp.bfloat16)
    low = (table - high.astype(np.float64)).astype(np.float32).astype(jnp.bfloat16)
    return high, low


def tables():
    counter = np.arange(WIN)
    angles = 2.0 * math.pi / WIN * (counter[:, None] * counter[None, :] % WIN)
    cos, sin = np.cos(angles), np.sin(angles)
    ramp = 1.0 - np.abs(counter - 15.5) / 16.0

    def rows(real, imag):
        return np.concatenate([real[:HALF], imag[:HALF], real[HALF:], imag[HALF:]])

    forward = np.concatenate(
        [rows(cos.T, sin.T).T, rows(-sin.T, cos.T).T], axis=0
    )
    high, low = hi_lo(forward)
    row_in = np.concatenate([high, high, low], axis=1)
    scale = ramp[:, None] / WIN
    backward = rows(
        np.concatenate([cos, -sin], axis=1) * scale, np.concatenate([sin, cos], axis=1) * scale
    )
    high, low = hi_lo(backward)
    row_out = np.concatenate([high, high, low], axis=1)
    four = np.eye(LANES // WIN)
    c, s = np.kron(four, cos), np.kron(four, sin)
    high, low = hi_lo(np.block([[c, -s], [s, c]]))
    col_in = np.concatenate([high, high, low], axis=0)
    taper = np.tile(ramp, LANES // WIN)[None, :] / WIN
    high, low = hi_lo(np.block([[c * taper, s * taper], [-s * taper, c * taper]]))
    col_out = np.concatenate([high, high, low], axis=0)
    ones = np.kron(four, np.ones((WIN, WIN)))
    ones = np.concatenate([ones, ones], axis=0).astype(jnp.bfloat16)
    return [row_in, col_in, col_out, row_out, ones]


def split(x):
    high = x.astype(BF16)
    return high, (x - high.astype(F32)).astype(BF16)


def split_rows(x):
    high, low = split(x)
    return jnp.concatenate([high, low, high], axis=0)


def split_cols(x):
    high, low = split(x)
    return jnp.concatenate([high, low, high], axis=1)


def dot(a, b):
    return jnp.dot(a, b, preferred_element_type=F32)


def halves(x, table):
    half = x.shape[0] // 2
    return jnp.concatenate(
        [dot(split_cols(x[:half]), table[...]), dot(split_cols(x[half:]), table[...])], axis=0
    )


def unit(phase):
    y = phase * 0.5
    t = y * y
    sine = -1.0 / 39916800.0
    for c in (1.0 / 362880.0, -1.0 / 5040.0, 1.0 / 120.0, -1.0 / 6.0, 1.0):
        sine = sine * t + c
    sine = sine * y
    cosine = 1.0 / 479001600.0
    for c in (-1.0 / 3628800.0, 1.0 / 40320.0, -1.0 / 720.0, 1.0 / 24.0, -0.5, 1.0):
        cosine = cosine * t + c
    return 1.0 - 2.0 * (sine * sine), 2.0 * (sine * cosine)


def to_lanes(tiles):
    return jnp.concatenate([tiles[j] for j in range(tiles.shape[0])], axis=1)


def to_tiles(wide):
    return jnp.stack(
        [wide[:, LANES * j : LANES * (j + 1)] for j in range(wide.shape[1] // LANES)]
    )


def kernel(
    n,
    tiles,
    phase_hbm,
    row_in_hbm,
    col_in_hbm,
    col_out_hbm,
    row_out_hbm,
    ones_hbm,
    out_ref,
    prof_ref,
    phase,
    row_in,
    col_in,
    col_out,
    row_out,
    ones,
    x,
    eo,
    rv,
    carry,
    pay,
    got,
    answer,
    load_sem,
    ph_send,
    ph_recv,
    up_send,
    up_recv,
    dn_send,
    dn_recv,
    pay_send,
    pay_recv,
    ans_send,
    ans_recv,
    relay,
):
    me = lax.axis_index("rows")
    has_above = me > 0
    has_below = me < n - 1

    def ring(offset):
        return {"rows": lax.rem(me + (offset + n), n)}

    def greet(sem, distance):
        for offset in (-distance, distance):
            pl.semaphore_signal(sem, inc=1, device_id=ring(offset), device_id_type=MESH)

    barrier = pltpu.get_barrier_semaphore()
    greet(barrier, 1)
    greet(barrier, 2)

    loads = [
        pltpu.make_async_copy(src, dst, load_sem.at[i])
        for i, (src, dst) in enumerate(
            [
                (phase_hbm, phase.at[0]),
                (row_in_hbm, row_in),
                (ones_hbm, ones),
                (col_in_hbm, col_in),
                (col_out_hbm, col_out),
                (row_out_hbm, row_out),
            ]
        )
    ]
    for load in loads:
        load.start()

    keep_below = jnp.where(has_below, 1.0, 0.0).astype(F32)

    @pl.when(jnp.logical_not(has_above))
    def _():
        rv[:, 0] = jnp.zeros(rv.shape[:1] + rv.shape[2:], F32)

    @pl.when(jnp.logical_not(has_below))
    def _():
        rv[:, 1] = jnp.zeros(rv.shape[:1] + rv.shape[2:], F32)
        phase[1] = jnp.zeros(phase.shape[1:], F32)

    x[tiles] = jnp.zeros(x.shape[1:], F32)
    loads[0].wait()
    pl.semaphore_wait(barrier, 4)

    stages = relay.shape[0]
    greet(relay.at[0], 2)

    def relay_step(s):
        if s < stages:
            pl.semaphore_wait(relay.at[s], 2)
            if s + 1 < stages:
                greet(relay.at[s + 1], 4 * 2 ** s)

    def phase_copy(c):
        first = PHASE_ENDS[c - 1] if c else 0
        cols = pl.ds(first * LANES, (PHASE_ENDS[c] - first) * LANES)
        return pltpu.make_async_remote_copy(
            src_ref=phase.at[0, :, cols],
            dst_ref=phase.at[1, :, cols],
            send_sem=ph_send,
            recv_sem=ph_recv.at[c],
            device_id={"rows": jnp.maximum(me - 1, 0)},
            device_id_type=MESH,
        )

    def span(it, c):
        ends = CHUNK_ENDS[it]
        return (ends[c - 1] if c else 0), ends[c]

    def up_copy(it, c):
        lo, hi = span(it, c)
        return pltpu.make_async_remote_copy(
            src_ref=eo.at[it, 0, pl.ds(lo, hi - lo)],
            dst_ref=rv.at[it, 1, pl.ds(lo, hi - lo)],
            send_sem=up_send,
            recv_sem=up_recv.at[it, c],
            device_id={"rows": jnp.maximum(me - 1, 0)},
            device_id_type=MESH,
        )

    def dn_copy(it, c):
        lo, hi = span(it, c)
        return pltpu.make_async_remote_copy(
            src_ref=eo.at[it, 1, pl.ds(lo, hi - lo)],
            dst_ref=rv.at[it, 0, pl.ds(lo, hi - lo)],
            send_sem=dn_send,
            recv_sem=dn_recv.at[it, c],
            device_id={"rows": jnp.minimum(me + 1, n - 1)},
            device_id_type=MESH,
        )

    @pl.when(has_above)
    def _():
        for c in range(len(PHASE_ENDS)):
            phase_copy(c).start()

    lane = lax.broadcasted_iota(jnp.int32, (1, 1, LANES), 2)

    def unit_tiles(row, lo, hi, scale=None):
        real, imag = unit(phase[row, :, lo * LANES : hi * LANES])
        if scale is not None:
            real, imag = real * scale, imag * scale
        return to_tiles(jnp.concatenate([real, imag], axis=0))

    x[0:tiles, 0:WIN] = unit_tiles(0, 0, tiles)
    for load in loads[1:]:
        load.wait()
    below_rows = lax.broadcasted_iota(jnp.int32, row_out.shape, 0) >= WIN
    row_out[...] = jnp.where(
        jnp.logical_and(below_rows, jnp.logical_not(has_below)),
        jnp.zeros(row_out.shape, BF16),
        row_out[...],
    )

    def arrive(it, c):
        if it == 0:
            lo, hi = (PHASE_ENDS[c - 1] if c else 0), PHASE_ENDS[c]

            @pl.when(has_below)
            def _():
                phase_copy(c).wait_recv()

            x[lo:hi, WIN:] = unit_tiles(1, lo, hi, keep_below)
            return hi
        lo, hi = span(it - 1, c)

        @pl.when(has_above)
        def _():
            dn_copy(it - 1, c).wait_recv()

        @pl.when(has_below)
        def _():
            up_copy(it - 1, c).wait_recv()

        x[lo:hi] = jnp.concatenate(
            [eo[it - 1, 0, lo:hi] + rv[it - 1, 0, lo:hi], eo[it - 1, 1, lo:hi] + rv[it - 1, 1, lo:hi]],
            axis=1,
        )
        return hi

    def residues(it, lo, hi):
        field = x[lo : hi + 1]
        last_row = lax.broadcasted_iota(jnp.int32, (1, HALF, 1), 1) == HALF - 1

        def lower(a, b):
            return jnp.where(last_row, b[:, 0:1], pltpu.roll(a, HALF - 1, 1))

        def right(a):
            return pltpu.roll(jnp.where(lane == 0, a[1:], a[:-1]), LANES - 1, 2)

        ar, ai = field[:, 0:HALF], field[:, HALF:WIN]
        dr = lower(ar, field[:, WIN : WIN + HALF])
        di = lower(ai, field[:, WIN + HALF :])
        pr, pi = ar[:-1] - right(dr), ai[:-1] - right(di)
        qr, qi = right(ar) - dr[:-1], right(ai) - di[:-1]
        loop = pi * qr - pr * qi
        loop = loop * loop
        loop = loop[:, 0:8] + loop[:, 8:HALF]
        sums = jnp.sum(loop, axis=2, keepdims=True)
        lanes = lax.broadcasted_iota(jnp.int32, (8, LANES), 1)
        total = jnp.zeros((8, LANES), F32)
        for j in range(hi - lo):
            total = jnp.where(lanes == it * tiles + lo + j, sums[j], total)
        return total

    def windows(it, lo, hi):
        count = hi - lo
        field = x[lo : hi + 1]
        y = to_tiles(dot(row_in[...], split_rows(to_lanes(field))))
        square = field * field
        square = sum(square[:, 8 * i : 8 * i + 8] for i in range(8))

        def both(tall):
            odd = pltpu.roll(jnp.where(lane < HALF, tall[1:], tall[:-1]), LANES - HALF, 2)
            return jnp.concatenate([tall[:-1], odd], axis=0)

        high, low = split(both(square).reshape(2 * count * 8, LANES))
        mean = dot(jnp.concatenate([high, low], axis=1), ones[...])
        mean = jnp.sum(mean.reshape(2 * count, 8, LANES), axis=1, keepdims=True)
        inverse = 1.0 / (mean + EPS)

        y = both(y)
        y = jnp.concatenate([y[:, 0:WIN], y[:, WIN:]], axis=2).reshape(2 * count * WIN, 2 * LANES)
        s = halves(y, col_in).reshape(2 * count, WIN, 2 * LANES)
        sr, si = s[:, :, 0:LANES], s[:, :, LANES:]
        gain = lax.rsqrt(lax.rsqrt((sr * sr + si * si) * inverse))
        s = jnp.concatenate([sr * gain, si * gain], axis=2).reshape(2 * count * WIN, 2 * LANES)
        s = halves(s, col_out).reshape(2 * count, WIN, 2 * LANES)
        s = jnp.concatenate([s[:, :, 0:LANES], s[:, :, LANES:]], axis=1)
        moved = pltpu.roll(s[count:], HALF, 2)
        if lo == 0:
            before = jnp.zeros((1, 2 * WIN, LANES), F32)
        else:
            before = carry[...][None]
        if hi < tiles:
            carry[...] = moved[count - 1]
        before = jnp.concatenate([before, moved[:-1]], axis=0)
        s = s[:count] + jnp.where(lane < HALF, before, moved)
        result = to_tiles(dot(row_out[...], split_rows(to_lanes(s))))
        eo[it, 0, lo:hi] = result[:, 0:WIN]
        eo[it, 1, lo:hi] = result[:, WIN:]

    def pay_copy(root):
        return pltpu.make_async_remote_copy(
            src_ref=pay,
            dst_ref=got.at[lax.rem(me - root + n, n)],
            send_sem=pay_send,
            recv_sem=pay_recv,
            device_id={"rows": root},
            device_id_type=MESH,
        )

    def answer_copy(i):
        return pltpu.make_async_remote_copy(
            src_ref=answer,
            dst_ref=answer,
            send_sem=ans_send,
            recv_sem=ans_recv,
            device_id={"rows": jnp.minimum(me + TELLERS * (i + 1), n - 1)},
            device_id_type=MESH,
        )

    chunks = len(PHASE_ENDS)
    payload = jnp.zeros((8, LANES), F32)
    relay_step(0)
    for it in range(ITERS - 1):
        for c in range(chunks):
            lo, hi = span(it, c)
            arrive(it, c)
            if it == 1 and c == 0:
                relay_step(2)
            windows(it, lo, hi)

            @pl.when(has_above)
            def _():
                up_copy(it, c).start()

            @pl.when(has_below)
            def _():
                dn_copy(it, c).start()

            if it == 0 and c == 0:
                relay_step(1)
        payload = payload + residues(it, 0, tiles)

    last = ITERS - 1
    for c in range(chunks):
        if c == chunks - 1:
            for s in range(3, stages):
                relay_step(s)
        arrive(last, c)
        payload = payload + residues(last, *span(last, c))
    pay[...] = jnp.sum(payload, axis=0, keepdims=True)
    for root in range(ROOTS):

        @pl.when(me != root)
        def _():
            pay_copy(root).start()

    for c in range(chunks):
        windows(last, *span(last, c))

        @pl.when(has_below)
        def _():
            dn_copy(last, c).start()

    for c in range(chunks):
        lo, hi = span(last, c)

        @pl.when(has_above)
        def _():
            dn_copy(last, c).wait_recv()

        final = to_lanes(eo[last, 0, lo:hi] + rv[last, 0, lo:hi])
        out_ref[0, :, lo * LANES : hi * LANES] = final[0:HALF]
        out_ref[1, :, lo * LANES : hi * LANES] = final[HALF:]
    def sent(ref, sem):
        pltpu.make_async_remote_copy(
            src_ref=ref,
            dst_ref=ref,
            send_sem=sem,
            recv_sem=pay_recv,
            device_id=ring(1),
            device_id_type=MESH,
        ).wait_send()

    @pl.when(has_above)
    def _():
        sent(phase.at[0], ph_send)
        sent(eo.at[pl.ds(0, last), 0], up_send)

    @pl.when(has_below)
    def _():
        sent(eo.at[pl.ds(0, ITERS), 1], dn_send)

    is_root = me < ROOTS
    is_teller = jnp.logical_and(is_root, me >= ROOTS - TELLERS)
    answers = (n - ROOTS) // TELLERS

    @pl.when(is_root)
    def _():
        sent(got.at[pl.ds(0, ROOTS - 1)], pay_send)
        others = got.at[pl.ds(1, n - 1)]
        pltpu.make_async_remote_copy(
            src_ref=others,
            dst_ref=others,
            send_sem=pay_send,
            recv_sem=pay_recv,
            device_id=ring(1),
            device_id_type=MESH,
        ).wait_recv()
        total = pay[...] + jnp.sum(got[1:n], axis=0)
        answer[...] = total * (1.0 / (n * HALF * LANES))

    @pl.when(is_teller)
    def _():
        for i in range(answers):
            answer_copy(i).start()

    @pl.when(jnp.logical_not(is_root))
    def _():
        sent(got.at[pl.ds(0, ROOTS)], pay_send)
        answer_copy(0).wait_recv()

    for it in range(ITERS):
        moved = answer[...] if it == 0 else pltpu.roll(answer[...], LANES - it * tiles, 1)
        prof_ref[it : it + 1, :] = moved[:, 0:tiles]

    @pl.when(is_teller)
    def _():
        sent(got.at[pl.ds(0, answers)], ans_send)


def finish_kernel(field, prof, field_out, prof_out, sems):
    copies = [
        pltpu.make_async_copy(field, field_out, sems.at[0]),
        pltpu.make_async_copy(prof, prof_out, sems.at[1]),
    ]
    for copy in copies:
        copy.start()
    for copy in copies:
        copy.wait()


def finish(field, prof):
    any_spec = pl.BlockSpec(memory_space=pl.ANY)
    vmem = pl.BlockSpec(memory_space=pltpu.VMEM)
    return pl.pallas_call(
        finish_kernel,
        out_shape=(
            jax.ShapeDtypeStruct(field.shape, F32),
            jax.ShapeDtypeStruct(prof.shape, F32),
        ),
        in_specs=[vmem, vmem],
        out_specs=(any_spec, any_spec),
        scratch_shapes=[pltpu.SemaphoreType.DMA((2,))],
        name="finish",
    )(field, prof)


def per_device(phase):
    n = lax.axis_size("rows")
    height, width = phase.shape
    tiles = width // LANES
    consts = [jnp.asarray(t) for t in tables()]
    stages = int(math.log2(n)) - 2
    chunks = len(PHASE_ENDS)
    dma = pltpu.SemaphoreType.DMA
    any_spec = pl.BlockSpec(memory_space=pl.ANY)
    results = pl.pallas_call(
        functools.partial(kernel, n, tiles),
        out_shape=(
            pltpu.VMEM((2, height, width), F32),
            pltpu.VMEM((ITERS, tiles), F32),
        ),
        in_specs=[any_spec] * 6,
        out_specs=(pl.BlockSpec(memory_space=pltpu.VMEM), pl.BlockSpec(memory_space=pltpu.VMEM)),
        scratch_shapes=[
            pltpu.VMEM((2, height, width), F32),
            *[pltpu.VMEM(c.shape, c.dtype) for c in consts[:4]],
            pltpu.VMEM(consts[4].shape, consts[4].dtype),
            pltpu.VMEM((tiles + 1, 2 * WIN, LANES), F32),
            pltpu.VMEM((ITERS, 2, tiles, WIN, LANES), F32),
            pltpu.VMEM((ITERS, 2, tiles, WIN, LANES), F32),
            pltpu.VMEM((2 * WIN, LANES), F32),
            pltpu.VMEM((1, LANES), F32),
            pltpu.VMEM((n, 1, LANES), F32),
            pltpu.VMEM((1, LANES), F32),
            dma((6,)),
            dma,
            dma((chunks,)),
            dma,
            dma((ITERS, chunks)),
            dma,
            dma((ITERS, chunks)),
            dma,
            dma,
            dma,
            dma,
            pltpu.SemaphoreType.REGULAR((stages,)),
        ],
        compiler_params=pltpu.CompilerParams(
            collective_id=0, has_side_effects=True, vmem_limit_bytes=60 << 20
        ),
        name="goldstein",
    )(phase, *consts)
    return finish(*[pltpu.with_memory_space_constraint(r, pltpu.VMEM) for r in results])


def solution(mesh):
    return jax.shard_map(
        per_device,
        mesh=mesh,
        in_specs=(P(("groups", "rows"), None),),
        out_specs=(P(None, ("groups", "rows"), None), P("groups", None)),
        check_vma=False,
    )
```

```python
import functools
import math

import jax
import jax.numpy as jnp
import numpy as np
from jax import lax
from jax.experimental import pallas as pl
from jax.experimental.pallas import tpu as pltpu
from jax.sharding import PartitionSpec as P

ITERS = 3
EPS = 1e-06
TINY = float(np.finfo(np.float32).tiny)
WIN = 32
HALF = 16
LANES = 128
F32 = jnp.float32
BF16 = jnp.bfloat16
MESH = pl.DeviceIdType.MESH
ROOTS = 8
TELLERS = 4

PHASE_ENDS = (7, 12, 16)
CHUNK_ENDS = ((6, 11, 16), (5, 10, 16), (4, 9, 16))


def hi_lo(table):
    high = table.astype(np.float32).astype(jnp.bfloat16)
    low = (table - high.astype(np.float64)).astype(np.float32).astype(jnp.bfloat16)
    return high, low


def tables():
    counter = np.arange(WIN)
    angles = 2.0 * math.pi / WIN * (counter[:, None] * counter[None, :] % WIN)
    cos, sin = np.cos(angles), np.sin(angles)
    ramp = 1.0 - np.abs(counter - 15.5) / 16.0

    def rows(real, imag):
        return np.concatenate([real[:HALF], imag[:HALF], real[HALF:], imag[HALF:]])

    forward = np.concatenate(
        [rows(cos.T, sin.T).T, rows(-sin.T, cos.T).T], axis=0
    )
    high, low = hi_lo(forward)
    row_in = np.concatenate([high, high, low], axis=1)
    scale = ramp[:, None] / WIN
    backward = rows(
        np.concatenate([cos, -sin], axis=1) * scale, np.concatenate([sin, cos], axis=1) * scale
    )
    high, low = hi_lo(backward)
    row_out = np.concatenate([high, high, low], axis=1)
    four = np.eye(LANES // WIN)
    c, s = np.kron(four, cos), np.kron(four, sin)
    high, low = hi_lo(np.block([[c, -s], [s, c]]))
    col_in = np.concatenate([high, high, low], axis=0)
    taper = np.tile(ramp, LANES // WIN)[None, :] / WIN
    high, low = hi_lo(np.block([[c * taper, s * taper], [-s * taper, c * taper]]))
    col_out = np.concatenate([high, high, low], axis=0)
    ones = np.kron(four, np.ones((WIN, WIN)))
    ones = np.concatenate([ones, ones], axis=0).astype(jnp.bfloat16)
    return [row_in, col_in, col_out, row_out, ones]


def split(x):
    high = x.astype(BF16)
    return high, (x - high.astype(F32)).astype(BF16)


def split_rows(x):
    high, low = split(x)
    return jnp.concatenate([high, low, high], axis=0)


def split_cols(x):
    high, low = split(x)
    return jnp.concatenate([high, low, high], axis=1)


def dot(a, b):
    return jnp.dot(a, b, preferred_element_type=F32)


def halves(x, table):
    half = x.shape[0] // 2
    return jnp.concatenate(
        [dot(split_cols(x[:half]), table[...]), dot(split_cols(x[half:]), table[...])], axis=0
    )


def unit(phase):
    y = phase * 0.5
    t = y * y
    sine = -1.0 / 39916800.0
    for c in (1.0 / 362880.0, -1.0 / 5040.0, 1.0 / 120.0, -1.0 / 6.0, 1.0):
        sine = sine * t + c
    sine = sine * y
    cosine = 1.0 / 479001600.0
    for c in (-1.0 / 3628800.0, 1.0 / 40320.0, -1.0 / 720.0, 1.0 / 24.0, -0.5, 1.0):
        cosine = cosine * t + c
    return 1.0 - 2.0 * (sine * sine), 2.0 * (sine * cosine)


def to_lanes(tiles):
    return jnp.concatenate([tiles[j] for j in range(tiles.shape[0])], axis=1)


def to_tiles(wide):
    return jnp.stack(
        [wide[:, LANES * j : LANES * (j + 1)] for j in range(wide.shape[1] // LANES)]
    )


def kernel(
    n,
    tiles,
    phase_hbm,
    row_in_hbm,
    col_in_hbm,
    col_out_hbm,
    row_out_hbm,
    ones_hbm,
    out_ref,
    prof_ref,
    phase,
    row_in,
    col_in,
    col_out,
    row_out,
    ones,
    x,
    eo,
    rv,
    carry,
    pay,
    got,
    answer,
    load_sem,
    ph_send,
    ph_recv,
    up_send,
    up_recv,
    dn_send,
    dn_recv,
    pay_send,
    pay_recv,
    ans_send,
    ans_recv,
    relay,
):
    me = lax.axis_index("rows")
    has_above = me > 0
    has_below = me < n - 1

    def ring(offset):
        return {"rows": lax.rem(me + (offset + n), n)}

    def greet(sem, distance):
        for offset in (-distance, distance):
            pl.semaphore_signal(sem, inc=1, device_id=ring(offset), device_id_type=MESH)

    barrier = pltpu.get_barrier_semaphore()
    greet(barrier, 1)
    greet(barrier, 2)

    loads = [
        pltpu.make_async_copy(src, dst, load_sem.at[i])
        for i, (src, dst) in enumerate(
            [
                (phase_hbm, phase.at[0]),
                (row_in_hbm, row_in),
                (ones_hbm, ones),
                (col_in_hbm, col_in),
                (col_out_hbm, col_out),
                (row_out_hbm, row_out),
            ]
        )
    ]
    for load in loads:
        load.start()

    keep_below = jnp.where(has_below, 1.0, 0.0).astype(F32)

    @pl.when(jnp.logical_not(has_above))
    def _():
        rv[:, 0] = jnp.zeros(rv.shape[:1] + rv.shape[2:], F32)

    @pl.when(jnp.logical_not(has_below))
    def _():
        rv[:, 1] = jnp.zeros(rv.shape[:1] + rv.shape[2:], F32)
        phase[1] = jnp.zeros(phase.shape[1:], F32)

    x[tiles] = jnp.zeros(x.shape[1:], F32)
    loads[0].wait()
    pl.semaphore_wait(barrier, 4)

    stages = relay.shape[0]
    greet(relay.at[0], 2)

    def relay_step(s):
        if s < stages:
            pl.semaphore_wait(relay.at[s], 2)
            if s + 1 < stages:
                greet(relay.at[s + 1], 4 * 2 ** s)

    def phase_copy(c):
        first = PHASE_ENDS[c - 1] if c else 0
        cols = pl.ds(first * LANES, (PHASE_ENDS[c] - first) * LANES)
        return pltpu.make_async_remote_copy(
            src_ref=phase.at[0, :, cols],
            dst_ref=phase.at[1, :, cols],
            send_sem=ph_send,
            recv_sem=ph_recv.at[c],
            device_id={"rows": jnp.maximum(me - 1, 0)},
            device_id_type=MESH,
        )

    def span(it, c):
        ends = CHUNK_ENDS[it]
        return (ends[c - 1] if c else 0), ends[c]

    def up_copy(it, c):
        lo, hi = span(it, c)
        return pltpu.make_async_remote_copy(
            src_ref=eo.at[it, 0, pl.ds(lo, hi - lo)],
            dst_ref=rv.at[it, 1, pl.ds(lo, hi - lo)],
            send_sem=up_send,
            recv_sem=up_recv.at[it, c],
            device_id={"rows": jnp.maximum(me - 1, 0)},
            device_id_type=MESH,
        )

    def dn_copy(it, c):
        lo, hi = span(it, c)
        return pltpu.make_async_remote_copy(
            src_ref=eo.at[it, 1, pl.ds(lo, hi - lo)],
            dst_ref=rv.at[it, 0, pl.ds(lo, hi - lo)],
            send_sem=dn_send,
            recv_sem=dn_recv.at[it, c],
            device_id={"rows": jnp.minimum(me + 1, n - 1)},
            device_id_type=MESH,
        )

    @pl.when(has_above)
    def _():
        for c in range(len(PHASE_ENDS)):
            phase_copy(c).start()

    lane = lax.broadcasted_iota(jnp.int32, (1, 1, LANES), 2)

    def unit_tiles(row, lo, hi, scale=None):
        real, imag = unit(phase[row, :, lo * LANES : hi * LANES])
        if scale is not None:
            real, imag = real * scale, imag * scale
        return to_tiles(jnp.concatenate([real, imag], axis=0))

    x[0:tiles, 0:WIN] = unit_tiles(0, 0, tiles)
    for load in loads[1:]:
        load.wait()
    below_rows = lax.broadcasted_iota(jnp.int32, row_out.shape, 0) >= WIN
    row_out[...] = jnp.where(
        jnp.logical_and(below_rows, jnp.logical_not(has_below)),
        jnp.zeros(row_out.shape, BF16),
        row_out[...],
    )

    def arrive(it, c):
        if it == 0:
            lo, hi = (PHASE_ENDS[c - 1] if c else 0), PHASE_ENDS[c]

            @pl.when(has_below)
            def _():
                phase_copy(c).wait_recv()

            x[lo:hi, WIN:] = unit_tiles(1, lo, hi, keep_below)
            return hi
        lo, hi = span(it - 1, c)

        @pl.when(has_above)
        def _():
            dn_copy(it - 1, c).wait_recv()

        @pl.when(has_below)
        def _():
            up_copy(it - 1, c).wait_recv()

        x[lo:hi] = jnp.concatenate(
            [eo[it - 1, 0, lo:hi] + rv[it - 1, 0, lo:hi], eo[it - 1, 1, lo:hi] + rv[it - 1, 1, lo:hi]],
            axis=1,
        )
        return hi

    def residues(it, lo, hi):
        field = x[lo : hi + 1]
        last_row = lax.broadcasted_iota(jnp.int32, (1, HALF, 1), 1) == HALF - 1

        def lower(a, b):
            return jnp.where(last_row, b[:, 0:1], pltpu.roll(a, HALF - 1, 1))

        def right(a):
            return pltpu.roll(jnp.where(lane == 0, a[1:], a[:-1]), LANES - 1, 2)

        ar, ai = field[:, 0:HALF], field[:, HALF:WIN]
        dr = lower(ar, field[:, WIN : WIN + HALF])
        di = lower(ai, field[:, WIN + HALF :])
        pr, pi = ar[:-1] - right(dr), ai[:-1] - right(di)
        qr, qi = right(ar) - dr[:-1], right(ai) - di[:-1]
        loop = pi * qr - pr * qi
        loop = loop * loop
        loop = loop[:, 0:8] + loop[:, 8:HALF]
        sums = jnp.sum(loop, axis=2, keepdims=True)
        lanes = lax.broadcasted_iota(jnp.int32, (8, LANES), 1)
        total = jnp.zeros((8, LANES), F32)
        for j in range(hi - lo):
            total = jnp.where(lanes == it * tiles + lo + j, sums[j], total)
        return total

    def windows(it, lo, hi):
        count = hi - lo
        field = x[lo : hi + 1]
        y = to_tiles(dot(row_in[...], split_rows(to_lanes(field))))
        square = field * field
        square = sum(square[:, 8 * i : 8 * i + 8] for i in range(8))

        def both(tall):
            odd = pltpu.roll(jnp.where(lane < HALF, tall[1:], tall[:-1]), LANES - HALF, 2)
            return jnp.concatenate([tall[:-1], odd], axis=0)

        high, low = split(both(square).reshape(2 * count * 8, LANES))
        mean = dot(jnp.concatenate([high, low], axis=1), ones[...])
        mean = jnp.sum(mean.reshape(2 * count, 8, LANES), axis=1, keepdims=True)
        inverse = 1.0 / (mean + EPS)

        y = both(y)
        y = jnp.concatenate([y[:, 0:WIN], y[:, WIN:]], axis=2).reshape(2 * count * WIN, 2 * LANES)
        s = halves(y, col_in).reshape(2 * count, WIN, 2 * LANES)
        sr, si = s[:, :, 0:LANES], s[:, :, LANES:]
        ratio = jnp.maximum((sr * sr + si * si) * inverse, TINY)
        gain = lax.rsqrt(lax.rsqrt(ratio))
        s = jnp.concatenate([sr * gain, si * gain], axis=2).reshape(2 * count * WIN, 2 * LANES)
        s = halves(s, col_out).reshape(2 * count, WIN, 2 * LANES)
        s = jnp.concatenate([s[:, :, 0:LANES], s[:, :, LANES:]], axis=1)
        moved = pltpu.roll(s[count:], HALF, 2)
        if lo == 0:
            before = jnp.zeros((1, 2 * WIN, LANES), F32)
        else:
            before = carry[...][None]
        if hi < tiles:
            carry[...] = moved[count - 1]
        before = jnp.concatenate([before, moved[:-1]], axis=0)
        s = s[:count] + jnp.where(lane < HALF, before, moved)
        result = to_tiles(dot(row_out[...], split_rows(to_lanes(s))))
        eo[it, 0, lo:hi] = result[:, 0:WIN]
        eo[it, 1, lo:hi] = result[:, WIN:]

    def pay_copy(root):
        return pltpu.make_async_remote_copy(
            src_ref=pay,
            dst_ref=got.at[lax.rem(me - root + n, n)],
            send_sem=pay_send,
            recv_sem=pay_recv,
            device_id={"rows": root},
            device_id_type=MESH,
        )

    def answer_copy(i):
        return pltpu.make_async_remote_copy(
            src_ref=answer,
            dst_ref=answer,
            send_sem=ans_send,
            recv_sem=ans_recv,
            device_id={"rows": jnp.minimum(me + TELLERS * (i + 1), n - 1)},
            device_id_type=MESH,
        )

    chunks = len(PHASE_ENDS)
    payload = jnp.zeros((8, LANES), F32)
    relay_step(0)
    for it in range(ITERS - 1):
        for c in range(chunks):
            lo, hi = span(it, c)
            arrive(it, c)
            if it == 1 and c == 0:
                relay_step(2)
            windows(it, lo, hi)

            @pl.when(has_above)
            def _():
                up_copy(it, c).start()

            @pl.when(has_below)
            def _():
                dn_copy(it, c).start()

            if it == 0 and c == 0:
                relay_step(1)
        payload = payload + residues(it, 0, tiles)

    last = ITERS - 1
    for c in range(chunks):
        if c == chunks - 1:
            for s in range(3, stages):
                relay_step(s)
        arrive(last, c)
        payload = payload + residues(last, *span(last, c))
    pay[...] = jnp.sum(payload, axis=0, keepdims=True)
    for root in range(ROOTS):

        @pl.when(me != root)
        def _():
            pay_copy(root).start()

    for c in range(chunks):
        windows(last, *span(last, c))

        @pl.when(has_below)
        def _():
            dn_copy(last, c).start()

    for c in range(chunks):
        lo, hi = span(last, c)

        @pl.when(has_above)
        def _():
            dn_copy(last, c).wait_recv()

        final = to_lanes(eo[last, 0, lo:hi] + rv[last, 0, lo:hi])
        out_ref[0, :, lo * LANES : hi * LANES] = final[0:HALF]
        out_ref[1, :, lo * LANES : hi * LANES] = final[HALF:]
    def sent(ref, sem):
        pltpu.make_async_remote_copy(
            src_ref=ref,
            dst_ref=ref,
            send_sem=sem,
            recv_sem=pay_recv,
            device_id=ring(1),
            device_id_type=MESH,
        ).wait_send()

    @pl.when(has_above)
    def _():
        sent(phase.at[0], ph_send)
        sent(eo.at[pl.ds(0, last), 0], up_send)

    @pl.when(has_below)
    def _():
        sent(eo.at[pl.ds(0, ITERS), 1], dn_send)

    is_root = me < ROOTS
    is_teller = jnp.logical_and(is_root, me >= ROOTS - TELLERS)
    answers = (n - ROOTS) // TELLERS

    @pl.when(is_root)
    def _():
        sent(got.at[pl.ds(0, ROOTS - 1)], pay_send)
        others = got.at[pl.ds(1, n - 1)]
        pltpu.make_async_remote_copy(
            src_ref=others,
            dst_ref=others,
            send_sem=pay_send,
            recv_sem=pay_recv,
            device_id=ring(1),
            device_id_type=MESH,
        ).wait_recv()
        total = pay[...] + jnp.sum(got[1:n], axis=0)
        answer[...] = total * (1.0 / (n * HALF * LANES))

    @pl.when(is_teller)
    def _():
        for i in range(answers):
            answer_copy(i).start()

    @pl.when(jnp.logical_not(is_root))
    def _():
        sent(got.at[pl.ds(0, ROOTS)], pay_send)
        answer_copy(0).wait_recv()

    for it in range(ITERS):
        moved = answer[...] if it == 0 else pltpu.roll(answer[...], LANES - it * tiles, 1)
        prof_ref[it : it + 1, :] = moved[:, 0:tiles]

    @pl.when(is_teller)
    def _():
        sent(got.at[pl.ds(0, answers)], ans_send)


def finish_kernel(field, prof, field_out, prof_out, sems):
    copies = [
        pltpu.make_async_copy(field, field_out, sems.at[0]),
        pltpu.make_async_copy(prof, prof_out, sems.at[1]),
    ]
    for copy in copies:
        copy.start()
    for copy in copies:
        copy.wait()


def finish(field, prof):
    any_spec = pl.BlockSpec(memory_space=pl.ANY)
    vmem = pl.BlockSpec(memory_space=pltpu.VMEM)
    return pl.pallas_call(
        finish_kernel,
        out_shape=(
            jax.ShapeDtypeStruct(field.shape, F32),
            jax.ShapeDtypeStruct(prof.shape, F32),
        ),
        in_specs=[vmem, vmem],
        out_specs=(any_spec, any_spec),
        scratch_shapes=[pltpu.SemaphoreType.DMA((2,))],
        name="finish",
    )(field, prof)


def per_device(phase):
    n = lax.axis_size("rows")
    height, width = phase.shape
    tiles = width // LANES
    consts = [jnp.asarray(t) for t in tables()]
    stages = int(math.log2(n)) - 2
    chunks = len(PHASE_ENDS)
    dma = pltpu.SemaphoreType.DMA
    any_spec = pl.BlockSpec(memory_space=pl.ANY)
    results = pl.pallas_call(
        functools.partial(kernel, n, tiles),
        out_shape=(
            pltpu.VMEM((2, height, width), F32),
            pltpu.VMEM((ITERS, tiles), F32),
        ),
        in_specs=[any_spec] * 6,
        out_specs=(pl.BlockSpec(memory_space=pltpu.VMEM), pl.BlockSpec(memory_space=pltpu.VMEM)),
        scratch_shapes=[
            pltpu.VMEM((2, height, width), F32),
            *[pltpu.VMEM(c.shape, c.dtype) for c in consts[:4]],
            pltpu.VMEM(consts[4].shape, consts[4].dtype),
            pltpu.VMEM((tiles + 1, 2 * WIN, LANES), F32),
            pltpu.VMEM((ITERS, 2, tiles, WIN, LANES), F32),
            pltpu.VMEM((ITERS, 2, tiles, WIN, LANES), F32),
            pltpu.VMEM((2 * WIN, LANES), F32),
            pltpu.VMEM((1, LANES), F32),
            pltpu.VMEM((n, 1, LANES), F32),
            pltpu.VMEM((1, LANES), F32),
            dma((6,)),
            dma,
            dma((chunks,)),
            dma,
            dma((ITERS, chunks)),
            dma,
            dma((ITERS, chunks)),
            dma,
            dma,
            dma,
            dma,
            pltpu.SemaphoreType.REGULAR((stages,)),
        ],
        compiler_params=pltpu.CompilerParams(
            collective_id=0, has_side_effects=True, vmem_limit_bytes=60 << 20
        ),
        name="goldstein",
    )(phase, *consts)
    return finish(*[pltpu.with_memory_space_constraint(r, pltpu.VMEM) for r in results])


def solution(mesh):
    return jax.shard_map(
        per_device,
        mesh=mesh,
        in_specs=(P(("groups", "rows"), None),),
        out_specs=(P(None, ("groups", "rows"), None), P("groups", None)),
        check_vma=False,
    )
```
